128 devices in a mesh: replica: 1, data2: 2 (over core), data: 64 (over z, y, x).
Axes of the slice: x: 4, y: 4, z: 4, core: 2. Of those that a mesh axis runs over, the one named last changes fastest.
Arguments:
- query_hidden: bfloat16 [512, 32, 768], P(('replica', 'data2', 'data'))
- doc_hidden: bfloat16 [512, 180, 768], P(('replica', 'data2', 'data'))
- w_proj: bfloat16 [768, 128], replicated
- query_mask: int32 [512, 32], P(('replica', 'data2', 'data'))
- doc_mask: int32 [512, 180], P(('replica', 'data2', 'data'))
- temperature: float32 [], replicated
Outputs:
- output 1: float32 [512], P(('replica', 'data2', 'data'))
- output 2: float32 [1], P('replica')
All inputs are finite; a program needn't handle non-finite values.
Results may differ from the reference program's by a relative error of at most 0.001.
Values are sent between devices in bfloat16 or wider.
A program may use at most 1 GiB of HBM per device.

```python
import jax
import jax.numpy as jnp
from jax import lax

BATCH = 512
QLEN = 32
DLEN = 180
HIDDEN = 768
PROJ = 128


def setup_inputs(seed: int = 0, part: int = 0) -> dict:
    root_key = jax.random.key(seed)
    key_common, key_parts = jax.random.split(root_key)
    part_key = jax.random.fold_in(key_parts, part)
    key_list = jax.random.split(part_key, 6)
    key_weight, key_temp = jax.random.split(key_common)
    shared = jax.random.normal(key_list[0], (HIDDEN,), jnp.float32)
    topic_vec = jax.random.normal(key_list[1], (BATCH, 1, HIDDEN), jnp.float32)
    concept = jax.random.normal(key_list[2], (BATCH, QLEN, HIDDEN), jnp.float32)
    token_noise = jax.random.normal(key_list[3], (BATCH, DLEN, HIDDEN), jnp.float32)
    query_lens = jax.random.randint(key_list[4], (BATCH,), QLEN // 2, QLEN + 1)
    doc_lens = jax.random.randint(key_list[5], (BATCH,), DLEN // 4, DLEN + 1)
    query_mask = (jnp.arange(QLEN)[None, :] < query_lens[:, None]).astype(jnp.int32)
    doc_mask = (jnp.arange(DLEN)[None, :] < doc_lens[:, None]).astype(jnp.int32)
    base_state = 0.6 * shared + 0.6 * topic_vec
    query_hidden = base_state + concept
    doc_concept = jnp.take(concept, jnp.arange(DLEN) % QLEN, axis=1)
    real_tok = base_state + 0.6 * doc_concept + 0.8 * token_noise
    pad_tok = 1.5 * shared + token_noise
    doc_hidden = jnp.where(doc_mask[:, :, None] > 0, real_tok, pad_tok)
    w_proj = jax.random.normal(key_weight, (HIDDEN, PROJ), jnp.float32) * HIDDEN ** -0.5
    temperature = QLEN * jax.random.uniform(key_temp, (), jnp.float32, 0.8, 1.25) / 8.0
    return {'query_hidden': query_hidden.astype(jnp.bfloat16), 'doc_hidden': doc_hidden.astype(jnp.bfloat16), 'w_proj': w_proj.astype(jnp.bfloat16), 'query_mask': query_mask, 'doc_mask': doc_mask, 'temperature': temperature}


def project_norm(hidden, w_proj):
    flat_states = hidden.reshape(-1, HIDDEN)
    projected = jnp.dot(flat_states, w_proj, preferred_element_type=jnp.float32)
    norm_len = jnp.sqrt(jnp.sum(projected * projected, axis=-1, keepdims=True))
    unit_vecs = projected / jnp.maximum(norm_len, 1e-12)
    return unit_vecs.astype(jnp.bfloat16).reshape(hidden.shape[0], hidden.shape[1], PROJ)


def reference(query_hidden, doc_hidden, w_proj, query_mask, doc_mask, temperature):
    q_vecs = project_norm(query_hidden, w_proj)
    p_vecs = project_norm(doc_hidden, w_proj).astype(jnp.float32)
    doc_valid = doc_mask[None, :, :] > 0

    def query_row(query_args):
        q_tok, q_weight = query_args
        similarity = jnp.einsum('tc,jsc->tjs', q_tok.astype(jnp.float32), p_vecs)
        best_match = jnp.max(jnp.where(doc_valid, similarity, -jnp.inf), axis=-1)
        return jnp.sum(q_weight.astype(jnp.float32)[:, None] * best_match, axis=0)

    scores = lax.map(query_row, (q_vecs, query_mask))
    logits = scores / temperature
    losses = jax.nn.logsumexp(logits, axis=1) - jnp.diagonal(logits)
    mean_loss = jnp.mean(losses).reshape(1)
    return losses, mean_loss
```

```python
import jax
import jax.numpy as jnp
from jax import lax
from jax.experimental import pallas as pl
from jax.experimental.pallas import tpu as pltpu
from jax.sharding import PartitionSpec as P

RING = 4
DIMS = ('z', 'y', 'x')
ORDERS = (('x', 'y', 'z'), ('y', 'z', 'x'), ('z', 'x', 'y'))
QPAD = 16


def unit_rows(hidden, w):
    projected = jnp.dot(hidden, w, preferred_element_type=jnp.float32)
    norm_len = jnp.sqrt(jnp.sum(projected * projected, axis=-1, keepdims=True))
    return projected / jnp.maximum(norm_len, 1e-12)


def as_column(row_mask, rows):
    cols = row_mask.shape[1]
    r = lax.broadcasted_iota(jnp.int32, (rows, cols), 0)
    c = lax.broadcasted_iota(jnp.int32, (rows, cols), 1)
    return jnp.sum(jnp.where(r == c, row_mask, 0.0), axis=1, keepdims=True)


def merge_docs(parts):
    rows = lax.broadcasted_iota(jnp.int32, parts[0].shape, 0)
    level = parts[::-1]
    for dist in (1, 2, 4):
        upper = (rows // dist) % 2 == 1
        merged = []
        for i in range(0, len(level), 2):
            a, b = level[i], level[i + 1]
            kept = jnp.where(upper, a, b)
            moved = pltpu.roll(jnp.where(upper, b, a), dist, 0)
            merged.append(jnp.maximum(kept, moved))
        level = merged
    return level[0]


def make_kernel(n_docs, dlen, n_q, qlen):
    doc_rows = -(-dlen // 8) * 8
    per_tile = QPAD // n_q
    chunks = qlen // per_tile
    total = 2 * RING ** 3 * n_q

    def kernel(qh_hbm, dh_hbm, w_hbm, qm_ref, dm_ref, temp_ref, loss_ref, mean_ref,
               qh, dh, w, qbuf, pbuf, acc, part, pieces, core_sum,
               load_sem, qsend, qrecv, psend, precv, rsend, rrecv, csend, crecv):
        core = lax.axis_index('data2')
        me = lax.axis_index('data')
        coord = {'z': me // (RING * RING), 'y': (me // RING) % RING, 'x': me % RING}

        def peer(dim, off):
            c = dict(coord)
            c[dim] = (coord[dim] + off) % RING
            return {'data': (c['z'] * RING + c['y']) * RING + c['x']}

        sibling = {'data2': 1 - core}
        barrier = pltpu.get_barrier_semaphore()
        for dim in DIMS:
            for off in (1, 2, 3):
                pl.semaphore_signal(barrier, inc=1, device_id=peer(dim, off))
        pl.semaphore_signal(barrier, inc=1, device_id=sibling)

        loads = [pltpu.make_async_copy(src, dst, load_sem.at[i])
                 for i, (src, dst) in enumerate(((w_hbm, w), (qh_hbm, qh), (dh_hbm, dh)))]
        for load in loads:
            load.start()

        loads[0].wait()
        loads[1].wait()
        w_val = w[...]
        q_rows = n_q * qlen
        q_unit = unit_rows(qh[...].reshape(q_rows, qh.shape[2]), w_val)
        qm = qm_ref[...].astype(jnp.float32)
        q_keep = jnp.concatenate([as_column(qm[i:i + 1], qlen) for i in range(n_q)], axis=0)
        q_vec = jnp.where(q_keep > 0, q_unit, 0.0).astype(jnp.bfloat16)
        r = lax.broadcasted_iota(jnp.int32, (q_rows, q_rows), 0)
        c = lax.broadcasted_iota(jnp.int32, (q_rows, q_rows), 1)
        order = jnp.where(c == (r % n_q) * qlen + r // n_q, 1.0, 0.0).astype(jnp.bfloat16)
        q_ord = jnp.dot(order, q_vec, preferred_element_type=jnp.float32).astype(jnp.bfloat16)
        q_ord = q_ord.reshape(chunks, QPAD, q_ord.shape[1])
        for k in range(chunks):
            qbuf[k, coord['z'], coord['y'], coord['x']] = q_ord[k]

        def gather_copy(k, phase, off):
            dims = ORDERS[k % 3]
            index = [k]
            for dim in DIMS:
                index.append(slice(None) if dim in dims[:phase] else coord[dim])
            ref = qbuf.at[tuple(index)]
            return pltpu.make_async_remote_copy(
                src_ref=ref, dst_ref=ref,
                send_sem=qsend.at[k, phase, off - 1], recv_sem=qrecv.at[k, phase, off - 1],
                device_id=peer(dims[phase], off))

        pl.semaphore_wait(barrier, 10)
        for k in range(chunks):
            for off in (1, 2, 3):
                gather_copy(k, 0, off).start()

        loads[2].wait()
        dm = dm_ref[...].astype(jnp.float32)
        lane = lax.broadcasted_iota(jnp.int32, dm.shape, 1)
        first = jnp.min(jnp.where(dm > 0, lane, dlen), axis=1, keepdims=True)
        pick = jnp.where(lane == first, 1.0, 0.0).astype(jnp.bfloat16)
        filled = []
        for j in range(n_docs):
            keep = as_column(dm[j:j + 1], doc_rows)
            unit = unit_rows(dh[j], w_val)
            unit = jnp.where(keep[:dlen] > 0, unit, 0.0).astype(jnp.bfloat16)
            valid_row = jnp.dot(pick[j:j + 1], unit, preferred_element_type=jnp.float32)
            unit = unit.astype(jnp.float32)
            pad = jnp.zeros((doc_rows - dlen, unit.shape[1]), jnp.float32)
            filled.append(jnp.where(keep > 0, jnp.concatenate([unit, pad], axis=0), valid_row))
        for h in range(n_docs // 2):
            both = jnp.concatenate(filled[2 * h:2 * h + 2], axis=0)
            pbuf[core, h] = both.astype(jnp.bfloat16)
        doc_copy = pltpu.make_async_remote_copy(
            src_ref=pbuf.at[core], dst_ref=pbuf.at[core], send_sem=psend, recv_sem=precv,
            device_id=sibling)
        doc_copy.start()

        for phase in (1, 2):
            for k in range(chunks):
                for off in (1, 2, 3):
                    gather_copy(k, phase - 1, off).wait_recv()
                for off in (1, 2, 3):
                    gather_copy(k, phase, off).start()
        doc_copy.wait_recv()

        for k in range(chunks):
            for off in (1, 2, 3):
                gather_copy(k, 2, off).wait_recv()
            for z in range(RING):
                q_tile = qbuf[k, z].reshape(RING * RING * QPAD, qbuf.shape[-1])
                parts = []
                for side in range(2):
                    for h in range(n_docs // 2):
                        sim = lax.dot_general(pbuf[side, h], q_tile, (((1,), (1,)), ((), ())),
                                              preferred_element_type=jnp.float32)
                        for d in range(2):
                            one = sim[d * doc_rows:(d + 1) * doc_rows]
                            parts.append(jnp.max(one.reshape(doc_rows // 8, 8, one.shape[1]), axis=0))
                best = merge_docs(parts)
                if k == 0:
                    acc[z] = best
                else:
                    acc[z] += best

        temp = temp_ref[0, 0]
        lanes = lax.broadcasted_iota(jnp.int32, (8, 256), 1)
        rows = lax.broadcasted_iota(jnp.int32, (8, 256), 0)
        lse = jnp.zeros((1, 256), jnp.float32)
        own = jnp.zeros((1, 256), jnp.float32)
        slot = lanes % QPAD
        is_own = (rows == core * n_docs + slot % n_q) & (
            lanes // QPAD == coord['y'] * RING + coord['x'])
        for z in range(RING):
            score = acc[z]
            shift = n_q
            while shift < QPAD:
                score = score + pltpu.roll(score, shift, 1)
                shift *= 2
            logits = score / temp
            top = jnp.max(logits, axis=0, keepdims=True)
            l = top + jnp.log(jnp.sum(jnp.exp(logits - top), axis=0, keepdims=True))
            d = jnp.sum(jnp.where(is_own & (coord['z'] == z), logits, 0.0), axis=0, keepdims=True)
            back = 256 - (QPAD - n_q) + z * n_q
            l = pltpu.roll(l, back % 256, 1)
            d = pltpu.roll(d, back % 256, 1)
            here = slot[:1] // n_q == z
            lse = jnp.where(here, l, lse)
            own = jnp.where(here, d, own)

        lse2 = jnp.concatenate([lse[:, :128], lse[:, 128:]], axis=0)
        own2 = jnp.concatenate([own[:, :128], own[:, 128:]], axis=0)

        def reduce_copy(phase, off):
            return pltpu.make_async_remote_copy(
                src_ref=part.at[phase], dst_ref=pieces.at[phase, off - 1],
                send_sem=rsend.at[phase, off - 1], recv_sem=rrecv.at[phase, off - 1],
                device_id=peer(DIMS[phase], off))

        for phase in range(3):
            part[phase, 0:2] = lse2
            part[phase, 2:4] = own2
            for off in (1, 2, 3):
                reduce_copy(phase, off).start()
            for off in (1, 2, 3):
                reduce_copy(phase, off).wait_recv()
            ls = [lse2] + [pieces[phase, o, 0:2] for o in range(3)]
            top = jnp.maximum(jnp.maximum(ls[0], ls[1]), jnp.maximum(ls[2], ls[3]))
            lse2 = top + jnp.log(sum(jnp.exp(l - top) for l in ls))
            own2 = own2 + sum(pieces[phase, o, 2:4] for o in range(3))

        losses = lse2 - own2
        plane = jnp.sum(jnp.sum(losses, axis=1, keepdims=True), axis=0, keepdims=True)
        core_sum[core] = jnp.broadcast_to(plane, core_sum.shape[1:])
        sum_copy = pltpu.make_async_remote_copy(
            src_ref=core_sum.at[core], dst_ref=core_sum.at[core], send_sem=csend, recv_sem=crecv,
            device_id=sibling)
        sum_copy.start()
        spot = (coord['y'] * RING + coord['x']) * QPAD + coord['z'] * n_q
        row = jnp.where(spot >= 128, losses[1:2], losses[0:1])
        row = pltpu.roll(jnp.broadcast_to(row, (8, 128)), (128 - spot % 128) % 128, 1)
        loss_ref[...] = row[0:1, :n_q]
        sum_copy.wait_recv()
        mean_ref[...] = ((core_sum[0] + core_sum[1]) / total)[0:1, 0:1]

        for k in range(chunks):
            for phase in range(3):
                for off in (1, 2, 3):
                    gather_copy(k, phase, off).wait_send()
        doc_copy.wait_send()
        for phase in range(3):
            for off in (1, 2, 3):
                reduce_copy(phase, off).wait_send()
        sum_copy.wait_send()

    return kernel


def solution(mesh):
    row_spec = P(('replica', 'data2', 'data'))
    tok_spec = P(('replica', 'data2', 'data'), None, None)
    mask_spec = P(('replica', 'data2', 'data'), None)

    def local_step(query_hidden, doc_hidden, w_proj, query_mask, doc_mask, temperature):
        n_q, qlen, hidden = query_hidden.shape
        n_docs, dlen, _ = doc_hidden.shape
        proj = w_proj.shape[1]
        doc_rows = -(-dlen // 8) * 8
        chunks = n_q * qlen // QPAD
        dma = pltpu.SemaphoreType.DMA
        losses, mean = pl.pallas_call(
            make_kernel(n_docs, dlen, n_q, qlen),
            out_shape=(jax.ShapeDtypeStruct((1, n_q), jnp.float32),
                       jax.ShapeDtypeStruct((1, 1), jnp.float32)),
            in_specs=[pl.BlockSpec(memory_space=pl.ANY)] * 3
            + [pl.BlockSpec(memory_space=pltpu.VMEM)] * 2
            + [pl.BlockSpec(memory_space=pltpu.SMEM)],
            out_specs=(pl.BlockSpec(memory_space=pltpu.VMEM), pl.BlockSpec(memory_space=pltpu.VMEM)),
            scratch_shapes=[
                pltpu.VMEM(query_hidden.shape, jnp.bfloat16),
                pltpu.VMEM(doc_hidden.shape, jnp.bfloat16),
                pltpu.VMEM(w_proj.shape, jnp.bfloat16),
                pltpu.VMEM((chunks, RING, RING, RING, QPAD, proj), jnp.bfloat16),
                pltpu.VMEM((2, n_docs // 2, 2 * doc_rows, proj), jnp.bfloat16),
                pltpu.VMEM((RING, 8, RING * RING * QPAD), jnp.float32),
                pltpu.VMEM((3, 4, 128), jnp.float32),
                pltpu.VMEM((3, 3, 4, 128), jnp.float32),
                pltpu.VMEM((2, 8, 128), jnp.float32),
                dma((3,)),
                dma((chunks, 3, 3)), dma((chunks, 3, 3)),
                dma, dma,
                dma((3, 3)), dma((3, 3)),
                dma, dma,
            ],
            compiler_params=pltpu.CompilerParams(collective_id=0, has_side_effects=True),
        )(query_hidden, doc_hidden, w_proj, query_mask, doc_mask, temperature.reshape(1, 1))
        return losses.reshape(n_q), mean.reshape(1)

    return jax.shard_map(local_step, mesh=mesh,
                         in_specs=(tok_spec, tok_spec, P(None, None), mask_spec, mask_spec, P()),
                         out_specs=(row_spec, P('replica')), check_vma=False)
```

```python
import jax
import jax.numpy as jnp
from jax import lax
from jax.experimental import pallas as pl
from jax.experimental.pallas import tpu as pltpu
from jax.sharding import PartitionSpec as P

RING = 4
SLOT = 16
OTHERS = (1, 2, 3)


def unit_rows(hidden, w):
    projected = jnp.dot(hidden, w, preferred_element_type=jnp.float32)
    norm_len = jnp.sqrt(jnp.sum(projected * projected, axis=-1, keepdims=True))
    return projected / jnp.maximum(norm_len, 1e-12)


def as_column(row_mask, rows):
    r = lax.broadcasted_iota(jnp.int32, (rows, rows), 0)
    c = lax.broadcasted_iota(jnp.int32, (rows, rows), 1)
    return jnp.sum(jnp.where(r == c, row_mask, 0.0), axis=1, keepdims=True)


def make_kernel(n_docs, dlen, n_q, qlen):
    doc_rows = n_docs * dlen
    head = doc_rows // 2 // 16 * 16 + 16
    halves = (pl.ds(0, head), pl.ds(head, doc_rows - head))
    chunks = n_q * qlen // SLOT
    color_of = (pl.ds(0, chunks // 2), pl.ds(chunks // 2, chunks // 2))
    plane = RING * RING * SLOT
    n_dev = 2 * RING ** 3

    def kernel(qh_hbm, dh_hbm, w_hbm, qm_ref, dm_ref, temp_ref, loss_ref, mean_ref,
               qh, dh, w, qbuf, pbuf, pieces,
               load_sem, qsend, qrecv, zsend, zrecv, fsend, frecv, dsend, drecv, rsend, rrecv):
        core = lax.axis_index('data2')
        me = lax.axis_index('data')
        z, y, x = me // (RING * RING), (me // RING) % RING, me % RING

        def at(dz, dy, dx):
            return {'data': (((z + dz) % RING) * RING + (y + dy) % RING) * RING + (x + dx) % RING}

        sibling = {'data2': 1 - core}
        up, down = at(1, 0, 0), at(RING - 1, 0, 0)
        barrier = pltpu.get_barrier_semaphore()
        near = [at(0, 0, o) for o in OTHERS] + [at(0, o, 0) for o in OTHERS] + [sibling]
        near += [at(o, 0, 0) for o in OTHERS] + [at(o, 0, 0) | sibling for o in OTHERS]
        for device in near:
            pl.semaphore_signal(barrier, inc=1, device_id=device)

        loads = [pltpu.make_async_copy(src, dst, load_sem.at[i])
                 for i, (src, dst) in enumerate(((w_hbm, w), (qh_hbm, qh), (dh_hbm, dh)))]
        for load in loads:
            load.start()

        q_rows = n_q * qlen
        qm = qm_ref[...].astype(jnp.float32)
        q_keep = jnp.concatenate([as_column(qm[i:i + 1], qlen) for i in range(n_q)], axis=0)
        r = lax.broadcasted_iota(jnp.int32, (q_rows, q_rows), 0)
        c = lax.broadcasted_iota(jnp.int32, (q_rows, q_rows), 1)
        order = jnp.where(c == (r % n_q) * qlen + r // n_q, 1.0, 0.0).astype(jnp.bfloat16)
        loads[0].wait()
        loads[1].wait()
        w_val = w[...]
        q_unit = unit_rows(qh[...].reshape(q_rows, qh.shape[2]), w_val)
        q_vec = jnp.where(q_keep > 0, q_unit, 0.0).astype(jnp.bfloat16)
        q_ord = jnp.dot(order, q_vec, preferred_element_type=jnp.float32).astype(jnp.bfloat16)
        q_ord = q_ord.reshape(chunks, SLOT, q_ord.shape[1])
        for k in range(chunks):
            qbuf[k, y, x] = q_ord[k]

        def line_copy(color, phase, off):
            along_x = color == phase
            rows = y if along_x or phase == 0 else slice(None)
            cols = x if not along_x or phase == 0 else slice(None)
            if phase == 1:
                rows, cols = (y, slice(None)) if color == 0 else (slice(None), x)
            ref = qbuf.at[color_of[color], rows, cols]
            return pltpu.make_async_remote_copy(
                src_ref=ref, dst_ref=ref,
                send_sem=qsend.at[color, phase, off - 1], recv_sem=qrecv.at[color, phase, off - 1],
                device_id=at(0, 0, off) if along_x else at(0, off, 0))

        pl.semaphore_wait(barrier, len(near))
        for color in range(2):
            for off in OTHERS:
                line_copy(color, 0, off).start()

        dm = dm_ref[...].astype(jnp.float32)
        lane = lax.broadcasted_iota(jnp.int32, dm.shape, 1)
        first = jnp.min(jnp.where(dm > 0, lane, dlen), axis=1, keepdims=True)
        r = lax.broadcasted_iota(jnp.int32, (n_docs, doc_rows), 1)
        d = lax.broadcasted_iota(jnp.int32, (n_docs, doc_rows), 0)
        pick = jnp.where(r == first * n_docs + d, 1.0, 0.0).astype(jnp.bfloat16)
        r = lax.broadcasted_iota(jnp.int32, (doc_rows, dlen), 0)
        c = lax.broadcasted_iota(jnp.int32, (doc_rows, dlen), 1)
        spread = jnp.where(r // n_docs == c, 1.0, 0.0).astype(jnp.bfloat16)
        keep = lax.dot_general(spread, dm.astype(jnp.bfloat16), (((1,), (1,)), ((), ())),
                               preferred_element_type=jnp.float32)
        r = lax.broadcasted_iota(jnp.int32, keep.shape, 0)
        c = lax.broadcasted_iota(jnp.int32, keep.shape, 1)
        keep = jnp.sum(jnp.where(r % n_docs == c, keep, 0.0), axis=1, keepdims=True)
        loads[2].wait()
        unit = unit_rows(dh[...].reshape(doc_rows, dh.shape[2]), w_val)
        unit = jnp.where(keep > 0, unit, 0.0).astype(jnp.bfloat16)
        valid = jnp.dot(pick, unit, preferred_element_type=jnp.float32)
        valid = jnp.concatenate([valid, valid], axis=0)
        valid = jnp.broadcast_to(valid[None], (doc_rows // 8, 8, valid.shape[1]))
        filled = jnp.where(keep > 0, unit.astype(jnp.float32), valid.reshape(doc_rows, valid.shape[2]))
        pbuf[z, core] = filled.astype(jnp.bfloat16)

        def doc_part(rel, h):
            return pbuf.at[(z + rel) % RING, core, halves[h]]

        def swap_copy(rel, h):
            ref = doc_part(rel, h)
            return pltpu.make_async_remote_copy(
                src_ref=ref, dst_ref=ref, send_sem=dsend.at[rel, h], recv_sem=drecv.at[rel, h],
                device_id=sibling)

        def z_copy(way, h):
            ref = doc_part(0, h)
            return pltpu.make_async_remote_copy(
                src_ref=ref, dst_ref=ref, send_sem=zsend.at[way, h], recv_sem=zrecv.at[way, h],
                device_id=down if way else up)

        def pass_copy(way):
            ref = doc_part(1 if way else RING - 1, way)
            return pltpu.make_async_remote_copy(
                src_ref=ref, dst_ref=ref, send_sem=fsend.at[way], recv_sem=frecv.at[way],
                device_id=down if way else up)

        for i in range(2):
            for way in range(2):
                z_copy(way, way ^ i).start()
        for h in range(2):
            swap_copy(0, h).start()

        for color in range(2):
            for off in OTHERS:
                line_copy(color, 0, off).wait_recv()
            for off in OTHERS:
                line_copy(color, 1, off).start()

        sub = lax.broadcasted_iota(jnp.int32, (8, plane), 0)

        def score(rel, side):
            total = None
            for k in range(chunks):
                sim = lax.dot_general(pbuf[(z + rel) % RING, side], qbuf[k].reshape(plane, qbuf.shape[-1]),
                                      (((1,), (1,)), ((), ())), preferred_element_type=jnp.float32)
                best = jnp.max(sim.reshape(doc_rows // 8, 8, plane), axis=0)
                best = jnp.maximum(best, pltpu.roll(best, 4, 0))
                total = best if total is None else total + best
            return total

        got = {}
        for way in range(2):
            z_copy(way, way).wait_recv()
            pass_copy(way).start()
            swap_copy(1 if way else 3, way).start()
        for color in range(2):
            for off in OTHERS:
                line_copy(color, 1, off).wait_recv()
        got[0, 0] = score(0, core)
        for way in range(2):
            z_copy(way, 1 - way).wait_recv()
            swap_copy(1 if way else 3, 1 - way).start()
        for h in range(2):
            swap_copy(0, h).wait_recv()
        got[0, 1] = score(0, 1 - core)
        for rel in (3, 1):
            got[rel, 0] = score(rel, core)
        for way in range(2):
            pass_copy(way).wait_recv()
            swap_copy(2, way).start()
        for rel in (3, 1):
            for h in range(2):
                swap_copy(rel, h).wait_recv()
            got[rel, 1] = score(rel, 1 - core)
        got[2, 0] = score(2, core)
        for h in range(2):
            swap_copy(2, h).wait_recv()
        got[2, 1] = score(2, 1 - core)

        temp = temp_ref[0, 0]
        logits = []
        for rel in range(RING):
            s = jnp.where(sub < 4, got[rel, 0], got[rel, 1])
            s = s + pltpu.roll(s, n_q, 1)
            s = s + pltpu.roll(s, 2 * n_q, 1)
            logits.append(s / temp)
        peak = jnp.maximum(jnp.maximum(logits[0], logits[1]), jnp.maximum(logits[2], logits[3]))
        peak = jnp.max(peak, axis=0, keepdims=True)
        mass = sum(jnp.exp(g - peak) for g in logits)
        part = peak + jnp.log(jnp.sum(mass, axis=0, keepdims=True))
        lanes = lax.broadcasted_iota(jnp.int32, (8, plane), 1)
        is_own = (sub == lanes % n_q) & (lanes // SLOT == y * RING + x) & (lanes % SLOT >= SLOT - n_q)
        own = jnp.sum(jnp.where(is_own, logits[0], 0.0), axis=0, keepdims=True)
        own_sum = jnp.sum(own, axis=1, keepdims=True)
        slot = lax.broadcasted_iota(jnp.int32, (1, 128), 1) % SLOT

        def fold(row):
            return jnp.where(slot >= 12, row[:, :128], pltpu.roll(row[:, 128:], 128 - n_q, 1))

        row = jnp.where(slot >= 8, fold(part), own_sum)
        own = fold(own)
        here = core * RING ** 3 + me
        pieces[here] = row

        def tell(step):
            other = {'data2': (core + step // RING ** 3) % 2, 'data': (me + step) % RING ** 3}
            return pltpu.make_async_remote_copy(
                src_ref=pieces.at[here], dst_ref=pieces.at[here], send_sem=rsend, recv_sem=rrecv,
                device_id=other)

        for step in range(1, n_dev):
            tell(step).start()
        everyone = pieces.at[pl.ds(0, n_dev - 1)]
        pltpu.make_async_copy(everyone, everyone, rrecv).wait()
        total = jnp.zeros((1, 1), jnp.float32)
        losses = jnp.zeros((1, 128), jnp.float32)
        for group in range(2 * RING):
            ls = [pieces[group * RING * RING + i] for i in range(RING * RING)]
            peak = ls[0]
            for l in ls[1:]:
                peak = jnp.maximum(peak, l)
            mass = sum(jnp.exp(l - peak) for l in ls)
            whole = peak + jnp.log(mass)
            total = total + jnp.sum(jnp.where(slot >= 8, whole, 0.0), axis=1, keepdims=True)
            total = total - sum(ls)[:, 0:1]
            losses = jnp.where(group == core * RING + z, whole, losses)
        losses = losses - own
        spot = (y * RING + x) % 8 * SLOT + jnp.where(y >= 2, 8, 12)
        losses = pltpu.roll(jnp.broadcast_to(losses, (8, 128)), (128 - spot) % 128, 1)
        loss_ref[...] = losses[0:1, :n_q]
        mean_ref[...] = total / (n_dev * n_q)

        for color in range(2):
            for phase in range(2):
                for off in OTHERS:
                    line_copy(color, phase, off).wait_send()
        for way in range(2):
            for h in range(2):
                z_copy(way, h).wait_send()
            pass_copy(way).wait_send()
        for rel in range(RING):
            for h in range(2):
                swap_copy(rel, h).wait_send()
        pltpu.make_async_copy(everyone, everyone, rsend).wait()

    return kernel


def solution(mesh):
    row_spec = P(('replica', 'data2', 'data'))
    tok_spec = P(('replica', 'data2', 'data'), None, None)
    mask_spec = P(('replica', 'data2', 'data'), None)

    def local_step(query_hidden, doc_hidden, w_proj, query_mask, doc_mask, temperature):
        n_q, qlen, hidden = query_hidden.shape
        n_docs, dlen, _ = doc_hidden.shape
        proj = w_proj.shape[1]
        chunks = n_q * qlen // SLOT
        dma = pltpu.SemaphoreType.DMA
        losses, mean = pl.pallas_call(
            make_kernel(n_docs, dlen, n_q, qlen),
            out_shape=(jax.ShapeDtypeStruct((1, n_q), jnp.float32),
                       jax.ShapeDtypeStruct((1, 1), jnp.float32)),
            in_specs=[pl.BlockSpec(memory_space=pl.ANY)] * 3
            + [pl.BlockSpec(memory_space=pltpu.VMEM)] * 2
            + [pl.BlockSpec(memory_space=pltpu.SMEM)],
            out_specs=(pl.BlockSpec(memory_space=pltpu.VMEM), pl.BlockSpec(memory_space=pltpu.VMEM)),
            scratch_shapes=[
                pltpu.VMEM(query_hidden.shape, jnp.bfloat16),
                pltpu.VMEM((dlen, n_docs, hidden), jnp.bfloat16),
                pltpu.VMEM(w_proj.shape, jnp.bfloat16),
                pltpu.VMEM((chunks, RING, RING, SLOT, proj), jnp.bfloat16),
                pltpu.VMEM((RING, 2, n_docs * dlen, proj), jnp.bfloat16),
                pltpu.VMEM((2 * RING ** 3, 1, 128), jnp.float32),
                dma((3,)),
                dma((2, 2, 3)), dma((2, 2, 3)),
                dma((2, 2)), dma((2, 2)),
                dma((2,)), dma((2,)),
                dma((RING, 2)), dma((RING, 2)),
                dma, dma,
            ],
            compiler_params=pltpu.CompilerParams(collective_id=0, has_side_effects=True),
        )(query_hidden, jnp.transpose(doc_hidden, (1, 0, 2)), w_proj, query_mask, doc_mask,
          temperature.reshape(1, 1))
        return losses.reshape(n_q), mean.reshape(1)

    return jax.shard_map(local_step, mesh=mesh,
                         in_specs=(tok_spec, tok_spec, P(None, None), mask_spec, mask_spec, P()),
                         out_specs=(row_spec, P('replica')), check_vma=False)
```

```python
import jax
import jax.numpy as jnp
from jax import lax
from jax.experimental import pallas as pl
from jax.experimental.pallas import tpu as pltpu
from jax.sharding import PartitionSpec as P

RING = 4
SLOT = 16
OTHERS = (1, 2, 3)


def unit_rows(hidden, w):
    projected = jnp.dot(hidden, w, preferred_element_type=jnp.float32)
    norm_len = jnp.sqrt(jnp.sum(projected * projected, axis=-1, keepdims=True))
    return projected / jnp.maximum(norm_len, 1e-12)


def as_column(row_mask, rows):
    r = lax.broadcasted_iota(jnp.int32, (rows, rows), 0)
    c = lax.broadcasted_iota(jnp.int32, (rows, rows), 1)
    return jnp.sum(jnp.where(r == c, row_mask, 0.0), axis=1, keepdims=True)


def far(*offsets):
    return sum(min(o, RING - o) for o in offsets)


def make_kernel(n_docs, dlen, n_q, qlen):
    doc_rows = n_docs * dlen
    head = doc_rows // 2 // 16 * 16 + 16
    halves = (pl.ds(0, head), pl.ds(head, doc_rows - head))
    chunks = n_q * qlen // SLOT
    steps = 4
    per_step = chunks // steps
    plane = RING * RING * SLOT
    n_dev = 2 * RING ** 3

    def kernel(qh_hbm, dh_hbm, w_hbm, qm_ref, dm_ref, temp_ref, loss_ref, mean_ref,
               qh, dh, w, qbuf, pbuf, pieces,
               load_sem, qsend, qrecv, zsend, zrecv, fsend, frecv, dsend, drecv, rsend, rrecv):
        core = lax.axis_index('data2')
        me = lax.axis_index('data')
        z, y, x = me // (RING * RING), (me // RING) % RING, me % RING

        zs = [(z + i) % RING * RING * RING for i in range(RING)]
        ys = [(y + i) % RING * RING for i in range(RING)]
        xs = [(x + i) % RING for i in range(RING)]

        def at(dz, dy, dx):
            return {'data': zs[dz] + ys[dy] + xs[dx]}

        sibling = {'data2': 1 - core}
        up, down = at(1, 0, 0), at(RING - 1, 0, 0)
        barrier = pltpu.get_barrier_semaphore()
        mates = [(dy, dx) for dy in range(RING) for dx in range(RING) if dy or dx]
        mates.sort(key=lambda m: -far(0, *m))
        near = [at(0, *m) for m in mates] + [sibling]
        near += [at(o, 0, 0) for o in OTHERS] + [at(o, 0, 0) | sibling for o in OTHERS]
        for device in near:
            pl.semaphore_signal(barrier, inc=1, device_id=device)

        loads = [pltpu.make_async_copy(src, dst, load_sem.at[i])
                 for i, (src, dst) in enumerate(((w_hbm, w), (qh_hbm, qh), (dh_hbm, dh)))]
        for load in loads:
            load.start()

        q_rows = n_q * qlen
        qm = qm_ref[...].astype(jnp.float32)
        q_keep = jnp.concatenate([as_column(qm[i:i + 1], qlen) for i in range(n_q)], axis=0)
        r = lax.broadcasted_iota(jnp.int32, (q_rows, q_rows), 0)
        c = lax.broadcasted_iota(jnp.int32, (q_rows, q_rows), 1)
        order = jnp.where(c == (r % n_q) * qlen + r // n_q, 1.0, 0.0).astype(jnp.bfloat16)
        loads[0].wait()
        loads[1].wait()
        w_val = w[...]
        q_unit = unit_rows(qh[...].reshape(q_rows, qh.shape[2]), w_val)
        q_vec = jnp.where(q_keep > 0, q_unit, 0.0).astype(jnp.bfloat16)
        q_ord = jnp.dot(order, q_vec, preferred_element_type=jnp.float32).astype(jnp.bfloat16)
        q_ord = q_ord.reshape(chunks, SLOT, q_ord.shape[1])
        for k in range(chunks):
            qbuf[k, y, x] = q_ord[k]

        def query_copy(step, mate):
            ref = qbuf.at[pl.ds(step * per_step, per_step), y, x]
            return pltpu.make_async_remote_copy(
                src_ref=ref, dst_ref=ref, send_sem=qsend.at[step], recv_sem=qrecv.at[step],
                device_id=at(0, *mate))

        def query_wait(step, sem):
            ref = qbuf.at[pl.ds(0, 5), pl.ds(0, 3), pl.ds(0, per_step)]
            pltpu.make_async_copy(ref, ref, sem.at[step]).wait()

        pl.semaphore_wait(barrier, len(near))
        for step in range(steps):
            for mate in mates:
                query_copy(step, mate).start()

        dm = dm_ref[...].astype(jnp.float32)
        lane = lax.broadcasted_iota(jnp.int32, dm.shape, 1)
        first = jnp.min(jnp.where(dm > 0, lane, dlen), axis=1, keepdims=True)
        r = lax.broadcasted_iota(jnp.int32, (n_docs, doc_rows), 1)
        d = lax.broadcasted_iota(jnp.int32, (n_docs, doc_rows), 0)
        pick = jnp.where(r == first * n_docs + d, 1.0, 0.0).astype(jnp.bfloat16)
        r = lax.broadcasted_iota(jnp.int32, (doc_rows, dlen), 0)
        c = lax.broadcasted_iota(jnp.int32, (doc_rows, dlen), 1)
        spread = jnp.where(r // n_docs == c, 1.0, 0.0).astype(jnp.bfloat16)
        keep = lax.dot_general(spread, dm.astype(jnp.bfloat16), (((1,), (1,)), ((), ())),
                               preferred_element_type=jnp.float32)
        r = lax.broadcasted_iota(jnp.int32, keep.shape, 0)
        c = lax.broadcasted_iota(jnp.int32, keep.shape, 1)
        keep = jnp.sum(jnp.where(r % n_docs == c, keep, 0.0), axis=1, keepdims=True)
        loads[2].wait()
        unit = unit_rows(dh[...].reshape(doc_rows, dh.shape[2]), w_val)
        unit = jnp.where(keep > 0, unit, 0.0).astype(jnp.bfloat16)
        valid = jnp.dot(pick, unit, preferred_element_type=jnp.float32)
        valid = jnp.concatenate([valid, valid], axis=0)
        valid = jnp.broadcast_to(valid[None], (doc_rows // 8, 8, valid.shape[1]))
        filled = jnp.where(keep > 0, unit.astype(jnp.float32), valid.reshape(doc_rows, valid.shape[2]))
        pbuf[z, core] = filled.astype(jnp.bfloat16)

        def doc_part(rel, h):
            return pbuf.at[(z + rel) % RING, core, halves[h]]

        def swap_copy(rel, h):
            ref = doc_part(rel, h)
            return pltpu.make_async_remote_copy(
                src_ref=ref, dst_ref=ref, send_sem=dsend.at[rel, h], recv_sem=drecv.at[rel, h],
                device_id=sibling)

        def z_copy(way, h):
            ref = doc_part(0, h)
            return pltpu.make_async_remote_copy(
                src_ref=ref, dst_ref=ref, send_sem=zsend.at[way, h], recv_sem=zrecv.at[way, h],
                device_id=down if way else up)

        def pass_copy(way):
            ref = doc_part(1 if way else RING - 1, way)
            return pltpu.make_async_remote_copy(
                src_ref=ref, dst_ref=ref, send_sem=fsend.at[way], recv_sem=frecv.at[way],
                device_id=down if way else up)

        for i in range(2):
            for way in range(2):
                z_copy(way, way ^ i).start()
        for h in range(2):
            swap_copy(0, h).start()

        sub = lax.broadcasted_iota(jnp.int32, (8, plane), 0)

        total = {}

        def score(rel, swapped, *which):
            docs = pbuf[(z + rel) % RING, 1 - core if swapped else core]
            for step in which:
                for k in range(step * per_step, (step + 1) * per_step):
                    sim = lax.dot_general(docs, qbuf[k].reshape(plane, qbuf.shape[-1]),
                                          (((1,), (1,)), ((), ())), preferred_element_type=jnp.float32)
                    best = jnp.max(sim.reshape(doc_rows // 8, 8, plane), axis=0)
                    best = jnp.maximum(best, pltpu.roll(best, 4, 0))
                    key = rel, swapped
                    total[key] = total[key] + best if key in total else best

        query_wait(0, qrecv)
        for way in range(2):
            z_copy(way, way).wait_recv()
            pass_copy(way).start()
            swap_copy(1 if way else 3, way).start()
        score(0, 0, 0)
        for h in range(2):
            swap_copy(0, h).wait_recv()
        score(0, 1, 0)
        query_wait(1, qrecv)
        score(0, 0, 1)
        score(0, 1, 1)
        for way in range(2):
            z_copy(way, 1 - way).wait_recv()
            swap_copy(1 if way else 3, 1 - way).start()
        score(3, 0, 0, 1)
        score(1, 0, 0, 1)
        query_wait(2, qrecv)
        score(0, 0, 2)
        score(0, 1, 2)
        score(3, 0, 2)
        score(1, 0, 2)
        for way in range(2):
            pass_copy(way).wait_recv()
            swap_copy(2, way).start()
        for rel in (3, 1):
            for h in range(2):
                swap_copy(rel, h).wait_recv()
            score(rel, 1, 0, 1, 2)
        query_wait(3, qrecv)
        for rel in (0, 3, 1):
            score(rel, 0, 3)
            score(rel, 1, 3)
        score(2, 0, 0, 1, 2, 3)
        for h in range(2):
            swap_copy(2, h).wait_recv()
        score(2, 1, 0, 1, 2, 3)

        temp = temp_ref[0, 0]
        logits = []
        for rel in range(RING):
            s = jnp.where(sub < 4, total[rel, 0], total[rel, 1])
            s = s + pltpu.roll(s, n_q, 1)
            s = s + pltpu.roll(s, 2 * n_q, 1)
            logits.append(s / temp)
        peak = jnp.maximum(jnp.maximum(logits[0], logits[1]), jnp.maximum(logits[2], logits[3]))
        peak = jnp.max(peak, axis=0, keepdims=True)
        mass = sum(jnp.exp(g - peak) for g in logits)
        part = peak + jnp.log(jnp.sum(mass, axis=0, keepdims=True))
        lanes = lax.broadcasted_iota(jnp.int32, (8, plane), 1)
        is_own = (sub == lanes % n_q) & (lanes // SLOT == y * RING + x) & (lanes % SLOT >= SLOT - n_q)
        own = jnp.sum(jnp.where(is_own, logits[0], 0.0), axis=0, keepdims=True)
        own_sum = jnp.sum(own, axis=1, keepdims=True)
        slot = lax.broadcasted_iota(jnp.int32, (1, 128), 1) % SLOT

        def fold(row):
            return jnp.where(slot >= 12, row[:, :128], pltpu.roll(row[:, 128:], 128 - n_q, 1))

        row = jnp.where(slot >= 8, fold(part), own_sum)
        own = fold(own)
        here = core * RING ** 3 + me
        pieces[here] = row

        def tell(across, dz, dy, dx):
            other = at(dz, dy, dx) | {'data2': 1 - core if across else core}
            return pltpu.make_async_remote_copy(
                src_ref=pieces.at[here], dst_ref=pieces.at[here], send_sem=rsend, recv_sem=rrecv,
                device_id=other)

        rest = [(a, i, j, k) for a in range(2) for i in range(RING) for j in range(RING) for k in range(RING)]
        for a, i, j, k in sorted(rest[1:], key=lambda o: -far(*o[1:])):
            tell(a, i, j, k).start()
        everyone = pieces.at[pl.ds(0, n_dev - 1)]
        pltpu.make_async_copy(everyone, everyone, rrecv).wait()
        answer = jnp.zeros((1, 1), jnp.float32)
        losses = jnp.zeros((1, 128), jnp.float32)
        for group in range(2 * RING):
            ls = [pieces[group * RING * RING + i] for i in range(RING * RING)]
            peak = ls[0]
            for l in ls[1:]:
                peak = jnp.maximum(peak, l)
            mass = sum(jnp.exp(l - peak) for l in ls)
            whole = peak + jnp.log(mass)
            answer = answer + jnp.sum(jnp.where(slot >= 8, whole, 0.0), axis=1, keepdims=True)
            answer = answer - sum(ls)[:, 0:1]
            losses = jnp.where(group == core * RING + z, whole, losses)
        losses = losses - own
        spot = (y * RING + x) % 8 * SLOT + jnp.where(y >= 2, 8, 12)
        losses = pltpu.roll(jnp.broadcast_to(losses, (8, 128)), (128 - spot) % 128, 1)
        loss_ref[...] = losses[0:1, :n_q]
        mean_ref[...] = answer / (n_dev * n_q)

        for step in range(steps):
            query_wait(step, qsend)
        for way in range(2):
            for h in range(2):
                z_copy(way, h).wait_send()
            pass_copy(way).wait_send()
        for rel in range(RING):
            for h in range(2):
                swap_copy(rel, h).wait_send()
        pltpu.make_async_copy(everyone, everyone, rsend).wait()

    return kernel


def hand_over(loss_in, mean_in, loss_ref, mean_ref):
    loss_ref[...] = loss_in[...]
    mean_ref[...] = mean_in[...]


def solution(mesh):
    row_spec = P(('replica', 'data2', 'data'))
    tok_spec = P(('replica', 'data2', 'data'), None, None)
    mask_spec = P(('replica', 'data2', 'data'), None)

    def local_step(query_hidden, doc_hidden, w_proj, query_mask, doc_mask, temperature):
        n_q, qlen, hidden = query_hidden.shape
        n_docs, dlen, _ = doc_hidden.shape
        proj = w_proj.shape[1]
        chunks = n_q * qlen // SLOT
        dma = pltpu.SemaphoreType.DMA
        losses, mean = pl.pallas_call(
            make_kernel(n_docs, dlen, n_q, qlen),
            out_shape=(jax.ShapeDtypeStruct((1, n_q), jnp.float32),
                       jax.ShapeDtypeStruct((1, 1), jnp.float32)),
            in_specs=[pl.BlockSpec(memory_space=pl.ANY)] * 3
            + [pl.BlockSpec(memory_space=pltpu.VMEM)] * 2
            + [pl.BlockSpec(memory_space=pltpu.SMEM)],
            out_specs=(pl.BlockSpec(memory_space=pltpu.VMEM), pl.BlockSpec(memory_space=pltpu.VMEM)),
            scratch_shapes=[
                pltpu.VMEM(query_hidden.shape, jnp.bfloat16),
                pltpu.VMEM((dlen, n_docs, hidden), jnp.bfloat16),
                pltpu.VMEM(w_proj.shape, jnp.bfloat16),
                pltpu.VMEM((chunks, RING, RING, SLOT, proj), jnp.bfloat16),
                pltpu.VMEM((RING, 2, n_docs * dlen, proj), jnp.bfloat16),
                pltpu.VMEM((2 * RING ** 3, 1, 128), jnp.float32),
                dma((3,)),
                dma((4,)), dma((4,)),
                dma((2, 2)), dma((2, 2)),
                dma((2,)), dma((2,)),
                dma((RING, 2)), dma((RING, 2)),
                dma, dma,
            ],
            compiler_params=pltpu.CompilerParams(collective_id=0, has_side_effects=True),
        )(query_hidden, jnp.transpose(doc_hidden, (1, 0, 2)), w_proj, query_mask, doc_mask,
          temperature.reshape(1, 1))
        losses, mean = pl.pallas_call(
            hand_over,
            out_shape=(jax.ShapeDtypeStruct((1, n_q), jnp.float32),
                       jax.ShapeDtypeStruct((1, 1), jnp.float32)))(losses, mean)
        return losses.reshape(n_q), mean.reshape(1)

    return jax.shard_map(local_step, mesh=mesh,
                         in_specs=(tok_spec, tok_spec, P(None, None), mask_spec, mask_spec, P()),
                         out_specs=(row_spec, P('replica')), check_vma=False)
```

```python
import jax
import jax.numpy as jnp
from jax import lax
from jax.experimental import pallas as pl
from jax.experimental.pallas import tpu as pltpu
from jax.sharding import PartitionSpec as P

RING = 4
SLOT = 16
OTHERS = (1, 2, 3)


def unit_rows(hidden, w):
    projected = jnp.dot(hidden, w, preferred_element_type=jnp.float32)
    norm_len = jnp.sqrt(jnp.sum(projected * projected, axis=-1, keepdims=True))
    return projected / jnp.maximum(norm_len, 1e-12)


def as_column(row_mask, rows):
    r = lax.broadcasted_iota(jnp.int32, (rows, rows), 0)
    c = lax.broadcasted_iota(jnp.int32, (rows, rows), 1)
    return jnp.sum(jnp.where(r == c, row_mask, 0.0), axis=1, keepdims=True)


def far(*offsets):
    return sum(min(o, RING - o) for o in offsets)


def make_kernel(n_docs, dlen, n_q, qlen):
    doc_rows = n_docs * dlen
    head = doc_rows // 2 // 16 * 16 + 16
    parts = (pl.ds(0, head), pl.ds(head, doc_rows - head), pl.ds(0, doc_rows))
    chunks = n_q * qlen // SLOT
    tiles = chunks // RING
    rounds = 4
    plane = RING * RING * SLOT
    n_dev = 2 * RING ** 3

    def kernel(qh_hbm, dh_hbm, w_hbm, qm_hbm, dm_hbm, temp_hbm, out_ref,
               qh, dh, w, qm_ref, dm_ref, temp_ref, qbuf, pbuf, sums, pieces,
               load_sem, qsend, qrecv, zsend, zrecv, fsend, frecv, dsend, drecv, rsend, rrecv):
        loads = [pltpu.make_async_copy(src, dst, load_sem.at[i]) for i, (src, dst) in enumerate((
            (w_hbm, w), (qh_hbm, qh), (qm_hbm, qm_ref), (dm_hbm, dm_ref), (dh_hbm, dh),
            (temp_hbm, temp_ref)))]
        for load in loads:
            load.start()

        core = lax.axis_index('data2')
        me = lax.axis_index('data')
        z, y, x = me // (RING * RING), (me // RING) % RING, me % RING

        zs = [(z + i) % RING * RING * RING for i in range(RING)]
        ys = [(y + i) % RING * RING for i in range(RING)]
        xs = [(x + i) % RING for i in range(RING)]

        def at(dz, dy, dx):
            return {'data': zs[dz] + ys[dy] + xs[dx]}

        sibling = {'data2': 1 - core}
        up, down = at(1, 0, 0), at(RING - 1, 0, 0)
        barrier = pltpu.get_barrier_semaphore()
        mates = [(dy, dx) for dy in range(RING) for dx in range(RING) if dy or dx]
        mates.sort(key=lambda m: (far(m[0]), -far(m[1])))
        near = [at(0, *m) for m in mates] + [sibling]
        near += [at(o, 0, 0) for o in OTHERS] + [at(o, 0, 0) | sibling for o in OTHERS]
        for device in near:
            pl.semaphore_signal(barrier, inc=1, device_id=device)

        q_rows = n_q * qlen
        r = lax.broadcasted_iota(jnp.int32, (q_rows, q_rows), 0)
        c = lax.broadcasted_iota(jnp.int32, (q_rows, q_rows), 1)
        order = jnp.where(c == (r % n_q) * qlen + r // n_q, 1.0, 0.0).astype(jnp.bfloat16)
        r = lax.broadcasted_iota(jnp.int32, (doc_rows, dlen), 0)
        c = lax.broadcasted_iota(jnp.int32, (doc_rows, dlen), 1)
        spread = jnp.where(r // n_docs == c, 1.0, 0.0).astype(jnp.bfloat16)
        loads[2].wait()
        qm = qm_ref[...].astype(jnp.float32)
        q_keep = jnp.concatenate([as_column(qm[i:i + 1], qlen) for i in range(n_q)], axis=0)

        loads[0].wait()
        loads[1].wait()
        w_val = w[...]
        q_unit = unit_rows(qh[...].reshape(q_rows, qh.shape[2]), w_val)
        q_vec = jnp.where(q_keep > 0, q_unit, 0.0).astype(jnp.bfloat16)
        q_ord = jnp.dot(order, q_vec, preferred_element_type=jnp.float32).astype(jnp.bfloat16)
        q_ord = q_ord.reshape(chunks, SLOT, q_ord.shape[1])
        for k in range(chunks):
            qbuf[k, y, x] = q_ord[k]

        def query_copy(mate, rnd):
            ref = qbuf.at[pl.ds(rnd * (chunks // rounds), chunks // rounds), y, x]
            return pltpu.make_async_remote_copy(
                src_ref=ref, dst_ref=ref, send_sem=qsend.at[mate[0]], recv_sem=qrecv.at[mate[0]],
                device_id=at(0, *mate))

        def query_wait(dy, sem):
            ref = qbuf.at[:, (y + RING - dy) % RING, pl.ds(0, RING if dy else RING - 1)]
            pltpu.make_async_copy(ref, ref, sem.at[dy]).wait()

        pl.semaphore_wait(barrier, len(near))
        for near_row in (0, 1, 2):
            for rnd in range(rounds):
                for mate in mates:
                    if far(mate[0]) == near_row:
                        query_copy(mate, rnd).start()

        loads[3].wait()
        loads[4].wait()
        dm = dm_ref[...].astype(jnp.float32)
        lane = lax.broadcasted_iota(jnp.int32, dm.shape, 1)
        first = jnp.min(jnp.where(dm > 0, lane, dlen), axis=1, keepdims=True)
        r = lax.broadcasted_iota(jnp.int32, (n_docs, doc_rows), 1)
        d = lax.broadcasted_iota(jnp.int32, (n_docs, doc_rows), 0)
        pick = jnp.where(r == first * n_docs + d, 1.0, 0.0).astype(jnp.bfloat16)
        keep = lax.dot_general(spread, dm.astype(jnp.bfloat16), (((1,), (1,)), ((), ())),
                               preferred_element_type=jnp.float32)
        r = lax.broadcasted_iota(jnp.int32, keep.shape, 0)
        c = lax.broadcasted_iota(jnp.int32, keep.shape, 1)
        keep = jnp.sum(jnp.where(r % n_docs == c, keep, 0.0), axis=1, keepdims=True)
        unit = unit_rows(dh[...].reshape(doc_rows, dh.shape[2]), w_val)
        unit = jnp.where(keep > 0, unit, 0.0).astype(jnp.bfloat16)
        valid = jnp.dot(pick, unit, preferred_element_type=jnp.float32)
        valid = jnp.concatenate([valid, valid], axis=0)
        valid = jnp.broadcast_to(valid[None], (doc_rows // 8, 8, valid.shape[1]))
        filled = jnp.where(keep > 0, unit.astype(jnp.float32), valid.reshape(doc_rows, valid.shape[2]))
        pbuf[z, core] = filled.astype(jnp.bfloat16)

        def doc_part(rel, h):
            return pbuf.at[(z + rel) % RING, core, parts[h]]

        def swap_copy(rel, h):
            ref = doc_part(rel, h)
            return pltpu.make_async_remote_copy(
                src_ref=ref, dst_ref=ref, send_sem=dsend.at[rel, h % 2], recv_sem=drecv.at[rel, h % 2],
                device_id=sibling)

        def z_copy(way, h):
            ref = doc_part(0, h)
            return pltpu.make_async_remote_copy(
                src_ref=ref, dst_ref=ref, send_sem=zsend.at[way, h], recv_sem=zrecv.at[way, h],
                device_id=down if way else up)

        def pass_copy(way):
            ref = doc_part(1 if way else RING - 1, way)
            return pltpu.make_async_remote_copy(
                src_ref=ref, dst_ref=ref, send_sem=fsend.at[way], recv_sem=frecv.at[way],
                device_id=down if way else up)

        for i in range(2):
            for way in range(2):
                z_copy(way, way ^ i).start()
        swap_copy(0, 2).start()

        sub = lax.broadcasted_iota(jnp.int32, (8, plane), 0)
        found, total = {}, {}

        def score(rel, swapped, part, rows):
            docs = pbuf[(z + rel) % RING, 1 - core if swapped else core, parts[part]]
            for dy in rows:
                for t in range(tiles):
                    q_tile = qbuf[t * RING:(t + 1) * RING, (y + RING - dy) % RING].reshape(plane, qbuf.shape[-1])
                    sim = lax.dot_general(docs, q_tile, (((1,), (1,)), ((), ())),
                                          preferred_element_type=jnp.float32)
                    best = jnp.max(sim.reshape(docs.shape[0] // 8, 8, plane), axis=0)
                    tile, key = (rel, swapped, dy, t), (rel, swapped, dy)
                    if part < 2 and tile not in found:
                        found[tile] = best
                        continue
                    if part < 2:
                        best = jnp.maximum(best, found[tile])
                    best = jnp.maximum(best, pltpu.roll(best, 4, 0))
                    total[key] = total[key] + best if key in total else best

        every, early = (0, 1, 2, 3), (0, 1)
        query_wait(0, qrecv)
        swap_copy(0, 2).wait_recv()
        score(0, 0, 2, (0,))
        score(0, 1, 2, (0,))
        for way in range(2):
            z_copy(way, way).wait_recv()
            pass_copy(way).start()
            swap_copy(1 if way else 3, way).start()
        score(3, 0, 0, (0,))
        score(1, 0, 1, (0,))
        query_wait(1, qrecv)
        score(0, 0, 2, (1,))
        score(0, 1, 2, (1,))
        score(3, 0, 0, (1,))
        score(1, 0, 1, (1,))
        for way in range(2):
            z_copy(way, 1 - way).wait_recv()
            swap_copy(1 if way else 3, 1 - way).start()
        for way in range(2):
            swap_copy(1 if way else 3, way).wait_recv()
        score(3, 1, 0, early)
        score(1, 1, 1, early)
        query_wait(3, qrecv)
        score(0, 0, 2, (3,))
        score(0, 1, 2, (3,))
        score(3, 0, 0, (3,))
        score(1, 0, 1, (3,))
        score(3, 1, 0, (3,))
        score(1, 1, 1, (3,))
        score(3, 0, 1, (0, 1, 3))
        score(1, 0, 0, (0, 1, 3))
        for way in range(2):
            pass_copy(way).wait_recv()
            swap_copy(2, way).start()
        query_wait(2, qrecv)
        for way in range(2):
            swap_copy(1 if way else 3, 1 - way).wait_recv()
        score(0, 0, 2, (2,))
        score(0, 1, 2, (2,))
        for way in range(2):
            rel = 1 if way else 3
            score(rel, 0, way, (2,))
            score(rel, 1, way, (2,))
            score(rel, 0, 1 - way, (2,))
            score(rel, 1, 1 - way, every)
        score(2, 0, 2, every)
        for h in range(2):
            swap_copy(2, h).wait_recv()
        score(2, 1, 2, every)

        half = lax.broadcasted_iota(jnp.int32, (8, 128), 1) < 64
        for rel in range(RING):
            for dy in range(RING):
                s = jnp.where(sub < 4, total[rel, 0, dy], total[rel, 1, dy])
                s = s[:, :128] + s[:, 128:]
                sums[rel, (y + RING - dy) % RING] = s + pltpu.roll(s, 64, 1)
        loads[5].wait()
        temp = temp_ref[...]
        logits = []
        for rel in range(RING):
            s = jnp.concatenate([jnp.where(half, sums[rel, i], sums[rel, i + 1]) for i in (0, 2)], axis=1)
            s = s + pltpu.roll(s, n_q, 1)
            s = s + pltpu.roll(s, 2 * n_q, 1)
            logits.append(s / temp)
        peak = jnp.maximum(jnp.maximum(logits[0], logits[1]), jnp.maximum(logits[2], logits[3]))
        peak = jnp.max(peak, axis=0, keepdims=True)
        mass = sum(jnp.exp(g - peak) for g in logits)
        part = peak + jnp.log(jnp.sum(mass, axis=0, keepdims=True))
        lanes = lax.broadcasted_iota(jnp.int32, (8, plane), 1)
        is_own = (sub == lanes % n_q) & (lanes // SLOT == y * RING + x) & (lanes % SLOT >= SLOT - n_q)
        own = jnp.sum(jnp.where(is_own, logits[0], 0.0), axis=0, keepdims=True)
        own_sum = jnp.sum(own, axis=1, keepdims=True)
        slot = lax.broadcasted_iota(jnp.int32, (1, 128), 1) % SLOT

        def fold(row):
            return jnp.where(slot >= 12, row[:, :128], pltpu.roll(row[:, 128:], 128 - n_q, 1))

        row = jnp.where(slot >= 8, fold(part), own_sum)
        own = fold(own)
        here = core * RING ** 3 + me
        pieces[here] = row

        def tell(across, dz, dy, dx):
            other = at(dz, dy, dx) | {'data2': 1 - core if across else core}
            return pltpu.make_async_remote_copy(
                src_ref=pieces.at[here], dst_ref=pieces.at[here], send_sem=rsend, recv_sem=rrecv,
                device_id=other)

        rest = [(a, i, j, k) for a in range(2) for i in range(RING) for j in range(RING) for k in range(RING)]
        for a, i, j, k in sorted(rest[1:], key=lambda o: -far(*o[1:])):
            tell(a, i, j, k).start()
        everyone = pieces.at[pl.ds(0, n_dev - 1)]
        pltpu.make_async_copy(everyone, everyone, rrecv).wait()
        ls = pieces[...].reshape(2 * RING, RING * RING, 128)
        peak = jnp.max(ls, axis=1, keepdims=True)
        mass = jnp.sum(jnp.exp(ls - peak), axis=1)
        whole = peak.reshape(2 * RING, 128) + jnp.log(mass)
        slot = lax.broadcasted_iota(jnp.int32, whole.shape, 1) % SLOT
        answer = jnp.where(slot >= 8, whole, 0.0)
        lane = lax.broadcasted_iota(jnp.int32, whole.shape, 1)
        answer = answer - jnp.where(lane == 0, jnp.sum(ls, axis=1), 0.0)
        answer = jnp.sum(jnp.sum(answer, axis=1, keepdims=True), axis=0, keepdims=True)
        group = lax.broadcasted_iota(jnp.int32, whole.shape, 0)
        losses = jnp.sum(jnp.where(group == core * RING + z, whole, 0.0), axis=0, keepdims=True)
        losses = losses - own
        spot = (y * RING + x) % 8 * SLOT + jnp.where(y >= 2, 8, 12)
        losses = pltpu.roll(jnp.broadcast_to(losses, (8, 128)), (128 - spot) % 128, 1)
        out_ref[0:1] = losses[0:1]
        out_ref[1:2] = jnp.broadcast_to(answer / (n_dev * n_q), (1, 128))

        for dy in range(RING):
            query_wait(dy, qsend)
        for way in range(2):
            for h in range(2):
                z_copy(way, h).wait_send()
            pass_copy(way).wait_send()
        swap_copy(0, 2).wait_send()
        for rel in OTHERS:
            for h in range(2):
                swap_copy(rel, h).wait_send()
        pltpu.make_async_copy(everyone, everyone, rsend).wait()

    return kernel


def hand_over(found_ref, loss_ref, mean_ref):
    loss_ref[...] = found_ref[0:1, :loss_ref.shape[1]]
    mean_ref[...] = found_ref[1:2, 0:1]


def solution(mesh):
    row_spec = P(('replica', 'data2', 'data'))
    tok_spec = P(('replica', 'data2', 'data'), None, None)
    mask_spec = P(('replica', 'data2', 'data'), None)

    def local_step(query_hidden, doc_hidden, w_proj, query_mask, doc_mask, temperature):
        n_q, qlen, hidden = query_hidden.shape
        n_docs, dlen, _ = doc_hidden.shape
        proj = w_proj.shape[1]
        chunks = n_q * qlen // SLOT
        dma = pltpu.SemaphoreType.DMA
        found = pl.pallas_call(
            make_kernel(n_docs, dlen, n_q, qlen),
            out_shape=jax.ShapeDtypeStruct((2, 128), jnp.float32),
            in_specs=[pl.BlockSpec(memory_space=pl.ANY)] * 6,
            out_specs=pl.BlockSpec(memory_space=pltpu.VMEM),
            scratch_shapes=[
                pltpu.VMEM(query_hidden.shape, jnp.bfloat16),
                pltpu.VMEM((dlen, n_docs, hidden), jnp.bfloat16),
                pltpu.VMEM(w_proj.shape, jnp.bfloat16),
                pltpu.VMEM(query_mask.shape, jnp.int32),
                pltpu.VMEM(doc_mask.shape, jnp.int32),
                pltpu.VMEM((1, 1), jnp.float32),
                pltpu.VMEM((chunks, RING, RING, SLOT, proj), jnp.bfloat16),
                pltpu.VMEM((RING, 2, n_docs * dlen, proj), jnp.bfloat16),
                pltpu.VMEM((RING, RING, 8, 128), jnp.float32),
                pltpu.VMEM((2 * RING ** 3, 1, 128), jnp.float32),
                dma((6,)),
                dma((4,)), dma((4,)),
                dma((2, 2)), dma((2, 2)),
                dma((2,)), dma((2,)),
                dma((RING, 2)), dma((RING, 2)),
                dma, dma,
            ],
            compiler_params=pltpu.CompilerParams(collective_id=0, has_side_effects=True),
        )(query_hidden, jnp.transpose(doc_hidden, (1, 0, 2)), w_proj, query_mask, doc_mask,
          temperature.reshape(1, 1))
        losses, mean = pl.pallas_call(
            hand_over,
            out_shape=(jax.ShapeDtypeStruct((1, n_q), jnp.float32),
                       jax.ShapeDtypeStruct((1, 1), jnp.float32)))(found)
        return losses.reshape(n_q), mean.reshape(1)

    return jax.shard_map(local_step, mesh=mesh,
                         in_specs=(tok_spec, tok_spec, P(None, None), mask_spec, mask_spec, P()),
                         out_specs=(row_spec, P('replica')), check_vma=False)
```

```python
import jax
import jax.numpy as jnp
from jax import lax
from jax.experimental import pallas as pl
from jax.experimental.pallas import tpu as pltpu
from jax.sharding import PartitionSpec as P

RING = 4
SLOT = 16
OTHERS = (1, 2, 3)


def unit_rows(hidden, w):
    projected = jnp.dot(hidden, w, preferred_element_type=jnp.float32)
    norm_len = jnp.sqrt(jnp.sum(projected * projected, axis=-1, keepdims=True))
    return projected / jnp.maximum(norm_len, 1e-12)


def as_column(row_mask, rows):
    r = lax.broadcasted_iota(jnp.int32, (rows, rows), 0)
    c = lax.broadcasted_iota(jnp.int32, (rows, rows), 1)
    return jnp.sum(jnp.where(r == c, row_mask, 0.0), axis=1, keepdims=True)


def far(*offsets):
    return sum(min(o, RING - o) for o in offsets)


def make_kernel(n_docs, dlen, n_q, qlen):
    doc_rows = n_docs * dlen
    head = doc_rows // 2 // 16 * 16 + 16
    parts = (pl.ds(0, head), pl.ds(head, doc_rows - head), pl.ds(0, doc_rows))
    chunks = n_q * qlen // SLOT
    tiles = chunks // RING
    rounds = 4
    plane = RING * RING * SLOT
    n_dev = 2 * RING ** 3

    def kernel(qh_hbm, dh_hbm, w_hbm, qm_hbm, dm_hbm, temp_hbm, out_ref,
               qh, dh, w, qm_ref, dm_ref, temp_ref, qbuf, pbuf, sums, pieces,
               load_sem, qsend, qrecv, zsend, zrecv, fsend, frecv, dsend, drecv, rsend, rrecv, ready):
        loads = [pltpu.make_async_copy(src, dst, load_sem.at[i]) for i, (src, dst) in enumerate((
            (w_hbm, w), (qh_hbm, qh), (qm_hbm, qm_ref), (dm_hbm, dm_ref), (dh_hbm, dh),
            (temp_hbm, temp_ref)))]
        for load in loads:
            load.start()

        core = lax.axis_index('data2')
        me = lax.axis_index('data')
        z, y, x = me // (RING * RING), (me // RING) % RING, me % RING

        zs = [(z + i) % RING * RING * RING for i in range(RING)]
        ys = [(y + i) % RING * RING for i in range(RING)]
        xs = [(x + i) % RING for i in range(RING)]

        def at(dz, dy, dx):
            return {'data': zs[dz] + ys[dy] + xs[dx]}

        sibling = {'data2': 1 - core}
        up, down = at(1, 0, 0), at(RING - 1, 0, 0)
        barrier = pltpu.get_barrier_semaphore()
        mates = [(dy, dx) for dy in range(RING) for dx in range(RING) if dy or dx]
        mates.sort(key=lambda m: (far(m[0]), -far(m[1])))
        near = [at(0, 0, o) for o in OTHERS] + [at(0, o, 0) for o in OTHERS] + [sibling]
        near += [at(o, 0, 0) for o in OTHERS] + [at(o, 0, 0) | sibling for o in OTHERS]
        for device in near:
            pl.semaphore_signal(barrier, inc=1, device_id=device)

        q_rows = n_q * qlen
        r = lax.broadcasted_iota(jnp.int32, (q_rows, q_rows), 0)
        c = lax.broadcasted_iota(jnp.int32, (q_rows, q_rows), 1)
        order = jnp.where(c == (r % n_q) * qlen + r // n_q, 1.0, 0.0).astype(jnp.bfloat16)
        r = lax.broadcasted_iota(jnp.int32, (doc_rows, dlen), 0)
        c = lax.broadcasted_iota(jnp.int32, (doc_rows, dlen), 1)
        spread = jnp.where(r // n_docs == c, 1.0, 0.0).astype(jnp.bfloat16)
        loads[2].wait()
        qm = qm_ref[...].astype(jnp.float32)
        q_keep = jnp.concatenate([as_column(qm[i:i + 1], qlen) for i in range(n_q)], axis=0)

        loads[0].wait()
        loads[1].wait()
        w_val = w[...]
        q_unit = unit_rows(qh[...].reshape(q_rows, qh.shape[2]), w_val)
        q_vec = jnp.where(q_keep > 0, q_unit, 0.0).astype(jnp.bfloat16)
        q_ord = jnp.dot(order, q_vec, preferred_element_type=jnp.float32).astype(jnp.bfloat16)
        q_ord = q_ord.reshape(chunks, SLOT, q_ord.shape[1])
        for k in range(chunks):
            qbuf[k, y, x] = q_ord[k]

        def query_copy(mate, rnd):
            ref = qbuf.at[pl.ds(rnd * (chunks // rounds), chunks // rounds), y, x]
            return pltpu.make_async_remote_copy(
                src_ref=ref, dst_ref=ref, send_sem=qsend.at[mate[0]], recv_sem=qrecv.at[mate[0]],
                device_id=at(0, *mate))

        def query_wait(dy, sem):
            ref = qbuf.at[:, (y + RING - dy) % RING, pl.ds(0, RING if dy else RING - 1)]
            pltpu.make_async_copy(ref, ref, sem.at[dy]).wait()

        loads[3].wait()
        loads[4].wait()
        dm = dm_ref[...].astype(jnp.float32)
        lane = lax.broadcasted_iota(jnp.int32, dm.shape, 1)
        first = jnp.min(jnp.where(dm > 0, lane, dlen), axis=1, keepdims=True)
        r = lax.broadcasted_iota(jnp.int32, (n_docs, doc_rows), 1)
        d = lax.broadcasted_iota(jnp.int32, (n_docs, doc_rows), 0)
        pick = jnp.where(r == first * n_docs + d, 1.0, 0.0).astype(jnp.bfloat16)
        keep = lax.dot_general(spread, dm.astype(jnp.bfloat16), (((1,), (1,)), ((), ())),
                               preferred_element_type=jnp.float32)
        r = lax.broadcasted_iota(jnp.int32, keep.shape, 0)
        c = lax.broadcasted_iota(jnp.int32, keep.shape, 1)
        keep = jnp.sum(jnp.where(r % n_docs == c, keep, 0.0), axis=1, keepdims=True)
        unit = unit_rows(dh[...].reshape(doc_rows, dh.shape[2]), w_val)
        unit = jnp.where(keep > 0, unit, 0.0).astype(jnp.bfloat16)
        valid = jnp.dot(pick, unit, preferred_element_type=jnp.float32)
        valid = jnp.concatenate([valid, valid], axis=0)
        valid = jnp.broadcast_to(valid[None], (doc_rows // 8, 8, valid.shape[1]))
        filled = jnp.where(keep > 0, unit.astype(jnp.float32), valid.reshape(doc_rows, valid.shape[2]))
        pbuf[z, core] = filled.astype(jnp.bfloat16)

        def doc_part(rel, h):
            return pbuf.at[(z + rel) % RING, core, parts[h]]

        def swap_copy(rel, h):
            ref = doc_part(rel, h)
            return pltpu.make_async_remote_copy(
                src_ref=ref, dst_ref=ref, send_sem=dsend.at[rel, h % 2], recv_sem=drecv.at[rel, h % 2],
                device_id=sibling)

        def z_copy(way, h):
            ref = doc_part(0, h)
            return pltpu.make_async_remote_copy(
                src_ref=ref, dst_ref=ref, send_sem=zsend.at[way, h], recv_sem=zrecv.at[way, h],
                device_id=down if way else up)

        def pass_copy(way):
            ref = doc_part(1 if way else RING - 1, way)
            return pltpu.make_async_remote_copy(
                src_ref=ref, dst_ref=ref, send_sem=fsend.at[way], recv_sem=frecv.at[way],
                device_id=down if way else up)

        pl.semaphore_wait(barrier, len(near))
        for off in OTHERS:
            pl.semaphore_signal(ready, inc=1, device_id=at(0, 0, off))
        for rnd in range(rounds):
            for mate in mates:
                if 0 in mate:
                    query_copy(mate, rnd).start()
        for i in range(2):
            for way in range(2):
                z_copy(way, way ^ i).start()
        swap_copy(0, 2).start()
        pl.semaphore_wait(ready, 3)
        for near_row in (1, 2):
            for rnd in range(rounds):
                for mate in mates:
                    if far(mate[0]) == near_row and mate[1]:
                        query_copy(mate, rnd).start()

        sub = lax.broadcasted_iota(jnp.int32, (8, plane), 0)
        found, total = {}, {}

        def score(rel, swapped, part, rows):
            docs = pbuf[(z + rel) % RING, 1 - core if swapped else core, parts[part]]
            for dy in rows:
                for t in range(tiles):
                    q_tile = qbuf[t * RING:(t + 1) * RING, (y + RING - dy) % RING].reshape(plane, qbuf.shape[-1])
                    sim = lax.dot_general(docs, q_tile, (((1,), (1,)), ((), ())),
                                          preferred_element_type=jnp.float32)
                    best = jnp.max(sim.reshape(docs.shape[0] // 8, 8, plane), axis=0)
                    tile, key = (rel, swapped, dy, t), (rel, swapped, dy)
                    if part < 2 and tile not in found:
                        found[tile] = best
                        continue
                    if part < 2:
                        best = jnp.maximum(best, found[tile])
                    best = jnp.maximum(best, pltpu.roll(best, 4, 0))
                    total[key] = total[key] + best if key in total else best

        every, early = (0, 1, 2, 3), (0, 1)
        query_wait(0, qrecv)
        swap_copy(0, 2).wait_recv()
        score(0, 0, 2, (0,))
        score(0, 1, 2, (0,))
        for way in range(2):
            z_copy(way, way).wait_recv()
            pass_copy(way).start()
            swap_copy(1 if way else 3, way).start()
        score(3, 0, 0, (0,))
        score(1, 0, 1, (0,))
        query_wait(1, qrecv)
        score(0, 0, 2, (1,))
        score(0, 1, 2, (1,))
        score(3, 0, 0, (1,))
        score(1, 0, 1, (1,))
        for way in range(2):
            z_copy(way, 1 - way).wait_recv()
            swap_copy(1 if way else 3, 1 - way).start()
        for way in range(2):
            swap_copy(1 if way else 3, way).wait_recv()
        score(3, 1, 0, early)
        score(1, 1, 1, early)
        query_wait(3, qrecv)
        score(0, 0, 2, (3,))
        score(0, 1, 2, (3,))
        score(3, 0, 0, (3,))
        score(1, 0, 1, (3,))
        score(3, 1, 0, (3,))
        score(1, 1, 1, (3,))
        score(3, 0, 1, (0, 1, 3))
        score(1, 0, 0, (0, 1, 3))
        for way in range(2):
            pass_copy(way).wait_recv()
            swap_copy(2, way).start()
        query_wait(2, qrecv)
        for way in range(2):
            swap_copy(1 if way else 3, 1 - way).wait_recv()
        score(0, 0, 2, (2,))
        score(0, 1, 2, (2,))
        for way in range(2):
            rel = 1 if way else 3
            score(rel, 0, way, (2,))
            score(rel, 1, way, (2,))
            score(rel, 0, 1 - way, (2,))
            score(rel, 1, 1 - way, every)
        score(2, 0, 2, every)
        for h in range(2):
            swap_copy(2, h).wait_recv()
        score(2, 1, 2, every)

        half = lax.broadcasted_iota(jnp.int32, (8, 128), 1) < 64
        for rel in range(RING):
            for dy in range(RING):
                s = jnp.where(sub < 4, total[rel, 0, dy], total[rel, 1, dy])
                s = s[:, :128] + s[:, 128:]
                sums[rel, (y + RING - dy) % RING] = s + pltpu.roll(s, 64, 1)
        loads[5].wait()
        temp = temp_ref[...]
        logits = []
        for rel in range(RING):
            s = jnp.concatenate([jnp.where(half, sums[rel, i], sums[rel, i + 1]) for i in (0, 2)], axis=1)
            s = s + pltpu.roll(s, n_q, 1)
            s = s + pltpu.roll(s, 2 * n_q, 1)
            logits.append(s / temp)
        peak = jnp.maximum(jnp.maximum(logits[0], logits[1]), jnp.maximum(logits[2], logits[3]))
        peak = jnp.max(peak, axis=0, keepdims=True)
        mass = sum(jnp.exp(g - peak) for g in logits)
        part = peak + jnp.log(jnp.sum(mass, axis=0, keepdims=True))
        lanes = lax.broadcasted_iota(jnp.int32, (8, plane), 1)
        is_own = (sub == lanes % n_q) & (lanes // SLOT == y * RING + x) & (lanes % SLOT >= SLOT - n_q)
        own = jnp.sum(jnp.where(is_own, logits[0], 0.0), axis=0, keepdims=True)
        own_sum = jnp.sum(own, axis=1, keepdims=True)
        slot = lax.broadcasted_iota(jnp.int32, (1, 128), 1) % SLOT

        def fold(row):
            return jnp.where(slot >= 12, row[:, :128], pltpu.roll(row[:, 128:], 128 - n_q, 1))

        row = jnp.where(slot >= 8, fold(part), own_sum)
        own = fold(own)
        here = core * RING ** 3 + me
        pieces[here] = row

        def tell(across, dz, dy, dx):
            other = at(dz, dy, dx) | {'data2': 1 - core if across else core}
            return pltpu.make_async_remote_copy(
                src_ref=pieces.at[here], dst_ref=pieces.at[here], send_sem=rsend, recv_sem=rrecv,
                device_id=other)

        rest = [(a, i, j, k) for a in range(2) for i in range(RING) for j in range(RING) for k in range(RING)]
        for a, i, j, k in sorted(rest[1:], key=lambda o: -far(*o[1:])):
            tell(a, i, j, k).start()
        everyone = pieces.at[pl.ds(0, n_dev - 1)]
        pltpu.make_async_copy(everyone, everyone, rrecv).wait()
        ls = pieces[...].reshape(2 * RING, RING * RING, 128)
        peak = jnp.max(ls, axis=1, keepdims=True)
        mass = jnp.sum(jnp.exp(ls - peak), axis=1)
        whole = peak.reshape(2 * RING, 128) + jnp.log(mass)
        slot = lax.broadcasted_iota(jnp.int32, whole.shape, 1) % SLOT
        answer = jnp.where(slot >= 8, whole, 0.0)
        lane = lax.broadcasted_iota(jnp.int32, whole.shape, 1)
        answer = answer - jnp.where(lane == 0, jnp.sum(ls, axis=1), 0.0)
        answer = jnp.sum(jnp.sum(answer, axis=1, keepdims=True), axis=0, keepdims=True)
        group = lax.broadcasted_iota(jnp.int32, whole.shape, 0)
        losses = jnp.sum(jnp.where(group == core * RING + z, whole, 0.0), axis=0, keepdims=True)
        losses = losses - own
        spot = (y * RING + x) % 8 * SLOT + jnp.where(y >= 2, 8, 12)
        losses = pltpu.roll(jnp.broadcast_to(losses, (8, 128)), (128 - spot) % 128, 1)
        out_ref[0:1] = losses[0:1]
        out_ref[1:2] = jnp.broadcast_to(answer / (n_dev * n_q), (1, 128))

        for dy in range(RING):
            query_wait(dy, qsend)
        for way in range(2):
            for h in range(2):
                z_copy(way, h).wait_send()
            pass_copy(way).wait_send()
        swap_copy(0, 2).wait_send()
        for rel in OTHERS:
            for h in range(2):
                swap_copy(rel, h).wait_send()
        pltpu.make_async_copy(everyone, everyone, rsend).wait()

    return kernel


def hand_over(found_ref, loss_ref, mean_ref):
    loss_ref[...] = found_ref[0:1, :loss_ref.shape[1]]
    mean_ref[...] = found_ref[1:2, 0:1]


def solution(mesh):
    row_spec = P(('replica', 'data2', 'data'))
    tok_spec = P(('replica', 'data2', 'data'), None, None)
    mask_spec = P(('replica', 'data2', 'data'), None)

    def local_step(query_hidden, doc_hidden, w_proj, query_mask, doc_mask, temperature):
        n_q, qlen, hidden = query_hidden.shape
        n_docs, dlen, _ = doc_hidden.shape
        proj = w_proj.shape[1]
        chunks = n_q * qlen // SLOT
        dma = pltpu.SemaphoreType.DMA
        found = pl.pallas_call(
            make_kernel(n_docs, dlen, n_q, qlen),
            out_shape=pltpu.VMEM((2, 128), jnp.float32),
            in_specs=[pl.BlockSpec(memory_space=pl.ANY)] * 6,
            out_specs=pl.BlockSpec(memory_space=pltpu.VMEM),
            scratch_shapes=[
                pltpu.VMEM(query_hidden.shape, jnp.bfloat16),
                pltpu.VMEM((dlen, n_docs, hidden), jnp.bfloat16),
                pltpu.VMEM(w_proj.shape, jnp.bfloat16),
                pltpu.VMEM(query_mask.shape, jnp.int32),
                pltpu.VMEM(doc_mask.shape, jnp.int32),
                pltpu.VMEM((1, 1), jnp.float32),
                pltpu.VMEM((chunks, RING, RING, SLOT, proj), jnp.bfloat16),
                pltpu.VMEM((RING, 2, n_docs * dlen, proj), jnp.bfloat16),
                pltpu.VMEM((RING, RING, 8, 128), jnp.float32),
                pltpu.VMEM((2 * RING ** 3, 1, 128), jnp.float32),
                dma((6,)),
                dma((4,)), dma((4,)),
                dma((2, 2)), dma((2, 2)),
                dma((2,)), dma((2,)),
                dma((RING, 2)), dma((RING, 2)),
                dma, dma,
                pltpu.SemaphoreType.REGULAR,
            ],
            compiler_params=pltpu.CompilerParams(collective_id=0, has_side_effects=True),
        )(query_hidden, jnp.transpose(doc_hidden, (1, 0, 2)), w_proj, query_mask, doc_mask,
          temperature.reshape(1, 1))
        losses, mean = pl.pallas_call(
            hand_over,
            out_shape=(jax.ShapeDtypeStruct((1, n_q), jnp.float32),
                       jax.ShapeDtypeStruct((1, 1), jnp.float32)),
            in_specs=[pl.BlockSpec(memory_space=pltpu.VMEM)],
            out_specs=(pl.BlockSpec(memory_space=pltpu.VMEM),) * 2,
            compiler_params=pltpu.CompilerParams(vmem_limit_bytes=2 ** 20))(found)
        return losses.reshape(n_q), mean.reshape(1)

    return jax.shard_map(local_step, mesh=mesh,
                         in_specs=(tok_spec, tok_spec, P(None, None), mask_spec, mask_spec, P()),
                         out_specs=(row_spec, P('replica')), check_vma=False)
```

```python
import jax
import jax.numpy as jnp
from jax import lax
from jax.experimental import pallas as pl
from jax.experimental.pallas import tpu as pltpu
from jax.sharding import PartitionSpec as P

RING = 4
SLOT = 16
OTHERS = (1, 2, 3)


def unit_rows(hidden, w):
    projected = jnp.dot(hidden, w, preferred_element_type=jnp.float32)
    norm_len = jnp.sqrt(jnp.sum(projected * projected, axis=-1, keepdims=True))
    return projected / jnp.maximum(norm_len, 1e-12)


def as_column(row_mask, rows):
    r = lax.broadcasted_iota(jnp.int32, (rows, rows), 0)
    c = lax.broadcasted_iota(jnp.int32, (rows, rows), 1)
    return jnp.sum(jnp.where(r == c, row_mask, 0.0), axis=1, keepdims=True)


def far(*offsets):
    return sum(min(o, RING - o) for o in offsets)


def make_kernel(n_docs, dlen, n_q, qlen):
    doc_rows = n_docs * dlen
    head = doc_rows // 2 // 16 * 16 + 16
    parts = (pl.ds(0, head), pl.ds(head, doc_rows - head), pl.ds(0, doc_rows))
    chunks = n_q * qlen // SLOT
    tiles = chunks // RING
    rounds = 4
    plane = RING * RING * SLOT
    n_dev = 2 * RING ** 3

    def kernel(qh_hbm, dh_hbm, w_hbm, qm_hbm, dm_hbm, temp_hbm, out_ref,
               qh, dh, w, qm_ref, dm_ref, temp_ref, qbuf, pbuf, sums, pieces,
               load_sem, qsend, qrecv, zsend, zrecv, fsend, frecv, dsend, drecv, rsend, rrecv, ready):
        loads = [pltpu.make_async_copy(src, dst, load_sem.at[i]) for i, (src, dst) in enumerate((
            (w_hbm, w), (qh_hbm, qh), (qm_hbm, qm_ref), (dm_hbm, dm_ref), (dh_hbm, dh),
            (temp_hbm, temp_ref)))]
        for load in loads:
            load.start()

        core = lax.axis_index('data2')
        me = lax.axis_index('data')
        z, y, x = me // (RING * RING), (me // RING) % RING, me % RING

        zs = [(z + i) % RING * RING * RING for i in range(RING)]
        ys = [(y + i) % RING * RING for i in range(RING)]
        xs = [(x + i) % RING for i in range(RING)]

        def at(dz, dy, dx):
            return {'data': zs[dz] + ys[dy] + xs[dx]}

        sibling = {'data2': 1 - core}
        up, down = at(1, 0, 0), at(RING - 1, 0, 0)
        barrier = pltpu.get_barrier_semaphore()
        mates = [(dy, dx) for dy in (0, 1, 3) for dx in range(RING) if dy or dx]
        mates.sort(key=lambda m: (far(m[0]), -far(m[1])))
        near = [at(0, 0, o) for o in OTHERS] + [at(0, o, 0) for o in OTHERS] + [sibling]
        near += [at(o, 0, 0) for o in OTHERS] + [at(o, 0, 0) | sibling for o in OTHERS]
        for device in near:
            pl.semaphore_signal(barrier, inc=1, device_id=device)

        q_rows = n_q * qlen
        r = lax.broadcasted_iota(jnp.int32, (q_rows, q_rows), 0)
        c = lax.broadcasted_iota(jnp.int32, (q_rows, q_rows), 1)
        order = jnp.where(c == (r % n_q) * qlen + r // n_q, 1.0, 0.0).astype(jnp.bfloat16)
        r = lax.broadcasted_iota(jnp.int32, (doc_rows, dlen), 0)
        c = lax.broadcasted_iota(jnp.int32, (doc_rows, dlen), 1)
        spread = jnp.where(r // n_docs == c, 1.0, 0.0).astype(jnp.bfloat16)
        loads[2].wait()
        qm = qm_ref[...].astype(jnp.float32)
        q_keep = jnp.concatenate([as_column(qm[i:i + 1], qlen) for i in range(n_q)], axis=0)

        loads[0].wait()
        loads[1].wait()
        w_val = w[...]
        q_unit = unit_rows(qh[...].reshape(q_rows, qh.shape[2]), w_val)
        q_vec = jnp.where(q_keep > 0, q_unit, 0.0).astype(jnp.bfloat16)
        q_ord = jnp.dot(order, q_vec, preferred_element_type=jnp.float32).astype(jnp.bfloat16)
        q_ord = q_ord.reshape(chunks, SLOT, q_ord.shape[1])
        for k in range(chunks):
            qbuf[k, y, x] = q_ord[k]

        def query_copy(mate, rnd):
            ref = qbuf.at[pl.ds(rnd * (chunks // rounds), chunks // rounds), y, x]
            sem = mate[0], rnd * tiles // rounds
            return pltpu.make_async_remote_copy(
                src_ref=ref, dst_ref=ref, send_sem=qsend.at[sem], recv_sem=qrecv.at[sem],
                device_id=at(0, *mate))

        def row_part(dy, t):
            return qbuf.at[pl.ds(t * RING, RING), (y + RING - dy) % RING]

        def query_wait(dy, t, sem):
            ref = row_part(dy, t).at[:, pl.ds(0, RING if dy else RING - 1)]
            pltpu.make_async_copy(ref, ref, sem.at[dy, t]).wait()

        def row_copy(dy):
            ref = row_part(dy, 0 if dy == 1 else 1)
            return pltpu.make_async_remote_copy(
                src_ref=ref, dst_ref=ref, send_sem=qsend.at[2, dy // 2], recv_sem=qrecv.at[2, dy // 2],
                device_id=at(0, dy, 0))

        loads[3].wait()
        loads[4].wait()
        dm = dm_ref[...].astype(jnp.float32)
        lane = lax.broadcasted_iota(jnp.int32, dm.shape, 1)
        first = jnp.min(jnp.where(dm > 0, lane, dlen), axis=1, keepdims=True)
        r = lax.broadcasted_iota(jnp.int32, (n_docs, doc_rows), 1)
        d = lax.broadcasted_iota(jnp.int32, (n_docs, doc_rows), 0)
        pick = jnp.where(r == first * n_docs + d, 1.0, 0.0).astype(jnp.bfloat16)
        keep = lax.dot_general(spread, dm.astype(jnp.bfloat16), (((1,), (1,)), ((), ())),
                               preferred_element_type=jnp.float32)
        r = lax.broadcasted_iota(jnp.int32, keep.shape, 0)
        c = lax.broadcasted_iota(jnp.int32, keep.shape, 1)
        keep = jnp.sum(jnp.where(r % n_docs == c, keep, 0.0), axis=1, keepdims=True)
        cut = dlen // 5
        unit = jnp.concatenate([
            unit_rows(dh[i:i + cut].reshape(cut * n_docs, dh.shape[2]), w[...])
            for i in range(0, dlen, cut)], axis=0)
        unit = jnp.where(keep > 0, unit, 0.0).astype(jnp.bfloat16)
        valid = jnp.dot(pick, unit, preferred_element_type=jnp.float32)
        valid = jnp.concatenate([valid, valid], axis=0)
        valid = jnp.broadcast_to(valid[None], (doc_rows // 8, 8, valid.shape[1]))
        filled = jnp.where(keep > 0, unit.astype(jnp.float32), valid.reshape(doc_rows, valid.shape[2]))
        pbuf[z, core] = filled.astype(jnp.bfloat16)

        def doc_part(rel, h):
            return pbuf.at[(z + rel) % RING, core, parts[h]]

        def swap_copy(rel, h):
            ref = doc_part(rel, h)
            return pltpu.make_async_remote_copy(
                src_ref=ref, dst_ref=ref, send_sem=dsend.at[rel, h % 2], recv_sem=drecv.at[rel, h % 2],
                device_id=sibling)

        def z_copy(way, h):
            ref = doc_part(0, h)
            return pltpu.make_async_remote_copy(
                src_ref=ref, dst_ref=ref, send_sem=zsend.at[way, h], recv_sem=zrecv.at[way, h],
                device_id=down if way else up)

        def pass_copy(way):
            ref = doc_part(1 if way else RING - 1, way)
            return pltpu.make_async_remote_copy(
                src_ref=ref, dst_ref=ref, send_sem=fsend.at[way], recv_sem=frecv.at[way],
                device_id=down if way else up)

        pl.semaphore_wait(barrier, len(near))
        for off in OTHERS:
            pl.semaphore_signal(ready, inc=1, device_id=at(0, 0, off))
        for i in range(2):
            for way in range(2):
                z_copy(way, way ^ i).start()
        for rnd in range(rounds):
            for mate in mates:
                if 0 in mate:
                    query_copy(mate, rnd).start()
        swap_copy(0, 2).start()
        pl.semaphore_wait(ready, 3)
        for i in range(tiles):
            for rnd in range(rounds // tiles):
                for mate in mates:
                    if 0 not in mate:
                        t = i if mate[0] == 1 else 1 - i
                        query_copy(mate, t * (rounds // tiles) + rnd).start()

        sub = lax.broadcasted_iota(jnp.int32, (8, plane), 0)
        found, total = {}, {}

        def score(rel, swapped, part, spots):
            docs = pbuf[(z + rel) % RING, 1 - core if swapped else core, parts[part]]
            for dy, t in spots:
                q_tile = row_part(dy, t)[...].reshape(plane, qbuf.shape[-1])
                sim = lax.dot_general(docs, q_tile, (((1,), (1,)), ((), ())),
                                      preferred_element_type=jnp.float32)
                best = jnp.max(sim.reshape(docs.shape[0] // 8, 8, plane), axis=0)
                tile, key = (rel, swapped, dy, t), (rel, swapped, dy)
                if part < 2 and tile not in found:
                    found[tile] = best
                    continue
                if part < 2:
                    best = jnp.maximum(best, found[tile])
                best = jnp.maximum(best, pltpu.roll(best, 4, 0))
                total[key] = total[key] + best if key in total else best

        sides, row0 = ((0, 3), (1, 1)), ((0, 0), (0, 1))
        near0, near1, row2 = ((1, 0), (3, 1)), ((1, 1), (3, 0)), ((2, 0), (2, 1))
        for t in range(tiles):
            query_wait(0, t, qrecv)
        swap_copy(0, 2).wait_recv()
        score(0, 0, 2, row0)
        score(0, 1, 2, row0)
        for way in range(2):
            z_copy(way, way).wait_recv()
            pass_copy(way).start()
            swap_copy(1 if way else 3, way).start()
        for way, rel in sides:
            score(rel, 0, way, row0)
        for way in range(2):
            z_copy(way, 1 - way).wait_recv()
            swap_copy(1 if way else 3, 1 - way).start()
        for way in range(2):
            swap_copy(1 if way else 3, way).wait_recv()
        for way, rel in sides:
            score(rel, 0, 1 - way, row0)
            score(rel, 1, way, row0)
        query_wait(1, 0, qrecv)
        row_copy(1).start()
        query_wait(3, 1, qrecv)
        row_copy(3).start()
        for spots in (near0, near1):
            if spots is near1:
                query_wait(1, 1, qrecv)
                query_wait(3, 0, qrecv)
            score(0, 0, 2, spots)
            score(0, 1, 2, spots)
            for way, rel in sides:
                score(rel, 0, way, spots)
                score(rel, 1, way, spots)
                score(rel, 0, 1 - way, spots)
        for way in range(2):
            pass_copy(way).wait_recv()
            swap_copy(2, way).start()
        for way in range(2):
            swap_copy(1 if way else 3, 1 - way).wait_recv()
        for way, rel in sides:
            score(rel, 1, 1 - way, row0 + near0 + near1)
        score(2, 0, 2, row0 + near0 + near1)
        row_copy(1).wait_recv()
        row_copy(3).wait_recv()
        for h in range(2):
            swap_copy(2, h).wait_recv()
        score(0, 0, 2, row2)
        score(0, 1, 2, row2)
        for way, rel in sides:
            for side in range(2):
                score(rel, side, way, row2)
                score(rel, side, 1 - way, row2)
        score(2, 0, 2, row2)
        score(2, 1, 2, row0 + near0 + near1 + row2)

        half = lax.broadcasted_iota(jnp.int32, (8, 128), 1) < 64
        for rel in range(RING):
            for dy in range(RING):
                s = jnp.where(sub < 4, total[rel, 0, dy], total[rel, 1, dy])
                s = s[:, :128] + s[:, 128:]
                sums[rel, (y + RING - dy) % RING] = s + pltpu.roll(s, 64, 1)
        loads[5].wait()
        temp = temp_ref[...]
        logits = []
        for rel in range(RING):
            s = jnp.concatenate([jnp.where(half, sums[rel, i], sums[rel, i + 1]) for i in (0, 2)], axis=1)
            s = s + pltpu.roll(s, n_q, 1)
            s = s + pltpu.roll(s, 2 * n_q, 1)
            logits.append(s / temp)
        peak = jnp.maximum(jnp.maximum(logits[0], logits[1]), jnp.maximum(logits[2], logits[3]))
        peak = jnp.max(peak, axis=0, keepdims=True)
        mass = sum(jnp.exp(g - peak) for g in logits)
        part = peak + jnp.log(jnp.sum(mass, axis=0, keepdims=True))
        lanes = lax.broadcasted_iota(jnp.int32, (8, plane), 1)
        is_own = (sub == lanes % n_q) & (lanes // SLOT == y * RING + x) & (lanes % SLOT >= SLOT - n_q)
        own = jnp.sum(jnp.where(is_own, logits[0], 0.0), axis=0, keepdims=True)
        own_sum = jnp.sum(own, axis=1, keepdims=True)
        slot = lax.broadcasted_iota(jnp.int32, (1, 128), 1) % SLOT

        def fold(row):
            return jnp.where(slot >= 12, row[:, :128], pltpu.roll(row[:, 128:], 128 - n_q, 1))

        row = jnp.where(slot >= 8, fold(part), own_sum)
        own = fold(own)
        here = core * RING ** 3 + me
        pieces[here] = row

        def tell(across, dz, dy, dx):
            other = at(dz, dy, dx) | {'data2': 1 - core if across else core}
            return pltpu.make_async_remote_copy(
                src_ref=pieces.at[here], dst_ref=pieces.at[here], send_sem=rsend, recv_sem=rrecv,
                device_id=other)

        rest = [(a, i, j, k) for a in range(2) for i in range(RING) for j in range(RING) for k in range(RING)]
        for a, i, j, k in sorted(rest[1:], key=lambda o: -far(*o[1:])):
            tell(a, i, j, k).start()
        everyone = pieces.at[pl.ds(0, n_dev - 1)]
        pltpu.make_async_copy(everyone, everyone, rrecv).wait()
        ls = pieces[...].reshape(2 * RING, RING * RING, 128)
        peak = jnp.max(ls, axis=1, keepdims=True)
        mass = jnp.sum(jnp.exp(ls - peak), axis=1)
        whole = peak.reshape(2 * RING, 128) + jnp.log(mass)
        slot = lax.broadcasted_iota(jnp.int32, whole.shape, 1) % SLOT
        answer = jnp.where(slot >= 8, whole, 0.0)
        lane = lax.broadcasted_iota(jnp.int32, whole.shape, 1)
        answer = answer - jnp.where(lane == 0, jnp.sum(ls, axis=1), 0.0)
        answer = jnp.sum(jnp.sum(answer, axis=1, keepdims=True), axis=0, keepdims=True)
        group = lax.broadcasted_iota(jnp.int32, whole.shape, 0)
        losses = jnp.sum(jnp.where(group == core * RING + z, whole, 0.0), axis=0, keepdims=True)
        losses = losses - own
        spot = (y * RING + x) % 8 * SLOT + jnp.where(y >= 2, 8, 12)
        losses = pltpu.roll(jnp.broadcast_to(losses, (8, 128)), (128 - spot) % 128, 1)
        out_ref[0:1] = losses[0:1]
        out_ref[1:2] = jnp.broadcast_to(answer / (n_dev * n_q), (1, 128))

        for t in range(tiles):
            for dy in (0, 1, 3):
                query_wait(dy, t, qsend)
        row_copy(1).wait_send()
        row_copy(3).wait_send()
        for way in range(2):
            for h in range(2):
                z_copy(way, h).wait_send()
            pass_copy(way).wait_send()
        swap_copy(0, 2).wait_send()
        for rel in OTHERS:
            for h in range(2):
                swap_copy(rel, h).wait_send()
        pltpu.make_async_copy(everyone, everyone, rsend).wait()

    return kernel


def hand_over(found_ref, loss_ref, mean_ref):
    loss_ref[...] = found_ref[0:1, :loss_ref.shape[1]]
    mean_ref[...] = found_ref[1:2, 0:1]


def solution(mesh):
    row_spec = P(('replica', 'data2', 'data'))
    tok_spec = P(('replica', 'data2', 'data'), None, None)
    mask_spec = P(('replica', 'data2', 'data'), None)

    def local_step(query_hidden, doc_hidden, w_proj, query_mask, doc_mask, temperature):
        n_q, qlen, hidden = query_hidden.shape
        n_docs, dlen, _ = doc_hidden.shape
        proj = w_proj.shape[1]
        chunks = n_q * qlen // SLOT
        dma = pltpu.SemaphoreType.DMA
        found = pl.pallas_call(
            make_kernel(n_docs, dlen, n_q, qlen),
            out_shape=pltpu.VMEM((2, 128), jnp.float32),
            in_specs=[pl.BlockSpec(memory_space=pl.ANY)] * 6,
            out_specs=pl.BlockSpec(memory_space=pltpu.VMEM),
            scratch_shapes=[
                pltpu.VMEM(query_hidden.shape, jnp.bfloat16),
                pltpu.VMEM((dlen, n_docs, hidden), jnp.bfloat16),
                pltpu.VMEM(w_proj.shape, jnp.bfloat16),
                pltpu.VMEM(query_mask.shape, jnp.int32),
                pltpu.VMEM(doc_mask.shape, jnp.int32),
                pltpu.VMEM((1, 1), jnp.float32),
                pltpu.VMEM((chunks, RING, RING, SLOT, proj), jnp.bfloat16),
                pltpu.VMEM((RING, 2, n_docs * dlen, proj), jnp.bfloat16),
                pltpu.VMEM((RING, RING, 8, 128), jnp.float32),
                pltpu.VMEM((2 * RING ** 3, 1, 128), jnp.float32),
                dma((6,)),
                dma((RING, 2)), dma((RING, 2)),
                dma((2, 2)), dma((2, 2)),
                dma((2,)), dma((2,)),
                dma((RING, 2)), dma((RING, 2)),
                dma, dma,
                pltpu.SemaphoreType.REGULAR,
            ],
            compiler_params=pltpu.CompilerParams(collective_id=0, has_side_effects=True),
        )(query_hidden, jnp.transpose(doc_hidden, (1, 0, 2)), w_proj, query_mask, doc_mask,
          temperature.reshape(1, 1))
        losses, mean = pl.pallas_call(
            hand_over,
            out_shape=(jax.ShapeDtypeStruct((1, n_q), jnp.float32),
                       jax.ShapeDtypeStruct((1, 1), jnp.float32)),
            in_specs=[pl.BlockSpec(memory_space=pltpu.VMEM)],
            out_specs=(pl.BlockSpec(memory_space=pltpu.VMEM),) * 2,
            compiler_params=pltpu.CompilerParams(vmem_limit_bytes=2 ** 20))(found)
        return losses.reshape(n_q), mean.reshape(1)

    return jax.shard_map(local_step, mesh=mesh,
                         in_specs=(tok_spec, tok_spec, P(None, None), mask_spec, mask_spec, P()),
                         out_specs=(row_spec, P('replica')), check_vma=False)
```

```python
import jax
import jax.numpy as jnp
from jax import lax
from jax.experimental import pallas as pl
from jax.experimental.pallas import tpu as pltpu
from jax.sharding import PartitionSpec as P

RING = 4
SLOT = 16
OTHERS = (1, 2, 3)
ROW0, NEAR0, NEAR1, ROW2, SIDE0, SIDE1, PASSED, SWAP0, SWAP1, SWAP2 = 0, (1, 2), 3, 4, (5, 6), 7, 8, 9, (10, 11), 12


def unit_rows(hidden, w):
    projected = jnp.dot(hidden, w, preferred_element_type=jnp.float32)
    norm_len = jnp.sqrt(jnp.sum(projected * projected, axis=-1, keepdims=True))
    return projected / jnp.maximum(norm_len, 1e-12)


def as_column(row_mask, rows):
    r = lax.broadcasted_iota(jnp.int32, (rows, rows), 0)
    c = lax.broadcasted_iota(jnp.int32, (rows, rows), 1)
    return jnp.sum(jnp.where(r == c, row_mask, 0.0), axis=1, keepdims=True)


def far(*offsets):
    return sum(min(o, RING - o) for o in offsets)


def make_kernel(n_docs, dlen, n_q, qlen):
    doc_rows = n_docs * dlen
    head = doc_rows // 2 // 16 * 16 + 16
    parts = (pl.ds(0, head), pl.ds(head, doc_rows - head), pl.ds(0, doc_rows))
    chunks = n_q * qlen // SLOT
    tiles = chunks // RING
    rounds = 4
    plane = RING * RING * SLOT
    n_dev = 2 * RING ** 3

    def kernel(qh_hbm, dh_hbm, w_hbm, qm_hbm, dm_hbm, temp_hbm, out_ref,
               qh, dh, w, qm_ref, dm_ref, temp_ref, qbuf, pbuf, sums, pieces,
               sent, load_sem, send, recv, rsend, rrecv, ready):
        loads = [pltpu.make_async_copy(src, dst, load_sem.at[i]) for i, (src, dst) in enumerate((
            (w_hbm, w), (qh_hbm, qh), (qm_hbm, qm_ref), (dm_hbm, dm_ref), (dh_hbm, dh),
            (temp_hbm, temp_ref)))]
        for load in loads:
            load.start()

        core = lax.axis_index('data2')
        me = lax.axis_index('data')
        z, y, x = me // (RING * RING), (me // RING) % RING, me % RING

        zs = [(z + i) % RING * RING * RING for i in range(RING)]
        ys = [(y + i) % RING * RING for i in range(RING)]
        xs = [(x + i) % RING for i in range(RING)]

        def at(dz, dy, dx):
            return {'data': zs[dz] + ys[dy] + xs[dx]}

        sibling = {'data2': 1 - core}
        up, down = at(1, 0, 0), at(RING - 1, 0, 0)
        barrier = pltpu.get_barrier_semaphore()
        mates = [(dy, dx) for dy in (0, 1, 3) for dx in range(RING) if dy or dx]
        mates.sort(key=lambda m: (far(m[0]), -far(m[1])))
        near = [at(0, 0, o) for o in OTHERS] + [at(0, o, 0) for o in OTHERS] + [sibling]
        near += [at(o, 0, 0) for o in OTHERS] + [at(o, 0, 0) | sibling for o in OTHERS]
        for device in near:
            pl.semaphore_signal(barrier, inc=1, device_id=device)

        q_rows = n_q * qlen
        r = lax.broadcasted_iota(jnp.int32, (q_rows, q_rows), 0)
        c = lax.broadcasted_iota(jnp.int32, (q_rows, q_rows), 1)
        order = jnp.where(c == (r % n_q) * qlen + r // n_q, 1.0, 0.0).astype(jnp.bfloat16)
        r = lax.broadcasted_iota(jnp.int32, (doc_rows, dlen), 0)
        c = lax.broadcasted_iota(jnp.int32, (doc_rows, dlen), 1)
        spread = jnp.where(r // n_docs == c, 1.0, 0.0).astype(jnp.bfloat16)
        loads[2].wait()
        qm = qm_ref[...].astype(jnp.float32)
        q_keep = jnp.concatenate([as_column(qm[i:i + 1], qlen) for i in range(n_q)], axis=0)

        loads[0].wait()
        loads[1].wait()
        w_val = w[...]
        q_unit = unit_rows(qh[...].reshape(q_rows, qh.shape[2]), w_val)
        q_vec = jnp.where(q_keep > 0, q_unit, 0.0).astype(jnp.bfloat16)
        q_ord = jnp.dot(order, q_vec, preferred_element_type=jnp.float32).astype(jnp.bfloat16)
        q_ord = q_ord.reshape(chunks, SLOT, q_ord.shape[1])
        for k in range(chunks):
            qbuf[k, y, x] = q_ord[k]

        def query_copy(mate, rnd):
            ref = qbuf.at[pl.ds(rnd * (chunks // rounds), chunks // rounds), y, x]
            dy, t = mate[0], rnd * tiles // rounds
            sem = ROW0 if dy == 0 else NEAR0[t] if t == dy // 2 else NEAR1
            return pltpu.make_async_remote_copy(
                src_ref=ref, dst_ref=ref, send_sem=send, recv_sem=recv.at[sem], device_id=at(0, *mate))

        def arrived(sem, ref):
            pltpu.make_async_copy(ref, ref, recv.at[sem]).wait()

        def row_part(dy, t):
            return qbuf.at[pl.ds(t * RING, RING), (y + RING - dy) % RING]

        def row_copy(dy):
            ref = row_part(dy, 0 if dy == 1 else 1)
            return pltpu.make_async_remote_copy(
                src_ref=ref, dst_ref=ref, send_sem=send, recv_sem=recv.at[ROW2],
                device_id=at(0, dy, 0))

        loads[3].wait()
        loads[4].wait()
        dm = dm_ref[...].astype(jnp.float32)
        lane = lax.broadcasted_iota(jnp.int32, dm.shape, 1)
        first = jnp.min(jnp.where(dm > 0, lane, dlen), axis=1, keepdims=True)
        r = lax.broadcasted_iota(jnp.int32, (n_docs, doc_rows), 1)
        d = lax.broadcasted_iota(jnp.int32, (n_docs, doc_rows), 0)
        pick = jnp.where(r == first * n_docs + d, 1.0, 0.0).astype(jnp.bfloat16)
        keep = lax.dot_general(spread, dm.astype(jnp.bfloat16), (((1,), (1,)), ((), ())),
                               preferred_element_type=jnp.float32)
        r = lax.broadcasted_iota(jnp.int32, keep.shape, 0)
        c = lax.broadcasted_iota(jnp.int32, keep.shape, 1)
        keep = jnp.sum(jnp.where(r % n_docs == c, keep, 0.0), axis=1, keepdims=True)
        cut = dlen // 5
        unit = jnp.concatenate([
            unit_rows(dh[i:i + cut].reshape(cut * n_docs, dh.shape[2]), w[...])
            for i in range(0, dlen, cut)], axis=0)
        unit = jnp.where(keep > 0, unit, 0.0).astype(jnp.bfloat16)
        valid = jnp.dot(pick, unit, preferred_element_type=jnp.float32)
        valid = jnp.concatenate([valid, valid], axis=0)
        valid = jnp.broadcast_to(valid[None], (doc_rows // 8, 8, valid.shape[1]))
        filled = jnp.where(keep > 0, unit.astype(jnp.float32), valid.reshape(doc_rows, valid.shape[2]))
        pbuf[z, core] = filled.astype(jnp.bfloat16)

        def doc_part(rel, h):
            return pbuf.at[(z + rel) % RING, core, parts[h]]

        def swap_copy(rel, h):
            ref = doc_part(rel, h)
            sem = SWAP0 if rel == 0 else SWAP2 if rel == 2 else SWAP1[rel // 2 == h]
            return pltpu.make_async_remote_copy(
                src_ref=ref, dst_ref=ref, send_sem=send, recv_sem=recv.at[sem], device_id=sibling)

        def z_copy(way, h):
            ref = doc_part(0, h)
            return pltpu.make_async_remote_copy(
                src_ref=ref, dst_ref=ref, send_sem=send, recv_sem=recv.at[SIDE0[way] if h == way else SIDE1],
                device_id=down if way else up)

        def pass_copy(way):
            ref = doc_part(1 if way else RING - 1, way)
            return pltpu.make_async_remote_copy(
                src_ref=ref, dst_ref=ref, send_sem=send, recv_sem=recv.at[PASSED],
                device_id=down if way else up)

        loads[5].wait()
        pl.semaphore_wait(barrier, len(near))
        for off in OTHERS:
            pl.semaphore_signal(ready, inc=1, device_id=at(0, 0, off))
        for i in range(2):
            for way in range(2):
                z_copy(way, way ^ i).start()
        for rnd in range(rounds):
            for mate in mates:
                if 0 in mate:
                    query_copy(mate, rnd).start()
        swap_copy(0, 2).start()
        pl.semaphore_wait(ready, 3)
        for i in range(tiles):
            for rnd in range(rounds // tiles):
                for mate in mates:
                    if 0 not in mate:
                        t = i if mate[0] == 1 else 1 - i
                        query_copy(mate, t * (rounds // tiles) + rnd).start()

        sub = lax.broadcasted_iota(jnp.int32, (8, plane), 0)
        found, total = {}, {}

        def score(rel, swapped, part, spots):
            docs = pbuf[(z + rel) % RING, 1 - core if swapped else core, parts[part]]
            for dy, t in spots:
                q_tile = row_part(dy, t)[...].reshape(plane, qbuf.shape[-1])
                sim = lax.dot_general(docs, q_tile, (((1,), (1,)), ((), ())),
                                      preferred_element_type=jnp.float32)
                best = jnp.max(sim.reshape(docs.shape[0] // 8, 8, plane), axis=0)
                tile, key = (rel, swapped, dy, t), (rel, swapped, dy)
                if part < 2 and tile not in found:
                    found[tile] = best
                    continue
                if part < 2:
                    best = jnp.maximum(best, found[tile])
                best = jnp.maximum(best, pltpu.roll(best, 4, 0))
                total[key] = total[key] + best if key in total else best

        sides, row0 = ((0, 3), (1, 1)), ((0, 0), (0, 1))
        near0, near1, row2 = ((1, 0), (3, 1)), ((1, 1), (3, 0)), ((2, 0), (2, 1))
        docs_ref, row_ref = pbuf.at[z, core], qbuf.at[:, y]
        arrived(ROW0, row_ref.at[:, pl.ds(0, RING - 1)])
        arrived(SWAP0, docs_ref)
        score(0, 0, 2, row0)
        score(0, 1, 2, row0)
        for way in range(2):
            z_copy(way, way).wait_recv()
            pass_copy(way).start()
            swap_copy(1 if way else 3, way).start()
        for way, rel in sides:
            score(rel, 0, way, row0)
        arrived(SIDE1, docs_ref)
        for way in range(2):
            swap_copy(1 if way else 3, 1 - way).start()
        arrived(SWAP1[0], docs_ref)
        for way, rel in sides:
            score(rel, 0, 1 - way, row0)
            score(rel, 1, way, row0)
        arrived(NEAR0[0], row_part(1, 0))
        row_copy(1).start()
        arrived(NEAR0[1], row_part(3, 1))
        row_copy(3).start()
        for spots in (near0, near1):
            if spots is near1:
                arrived(NEAR1, row_ref)
            score(0, 0, 2, spots)
            score(0, 1, 2, spots)
            for way, rel in sides:
                score(rel, 0, way, spots)
                score(rel, 1, way, spots)
                score(rel, 0, 1 - way, spots)
        arrived(PASSED, docs_ref)
        for way in range(2):
            swap_copy(2, way).start()
        arrived(SWAP1[1], docs_ref)
        for way, rel in sides:
            score(rel, 1, 1 - way, row0 + near0 + near1)
        score(2, 0, 2, row0 + near0 + near1)
        arrived(ROW2, row_ref)
        arrived(SWAP2, docs_ref)
        score(0, 0, 2, row2)
        score(0, 1, 2, row2)
        for way, rel in sides:
            for side in range(2):
                score(rel, side, way, row2)
                score(rel, side, 1 - way, row2)
        score(2, 0, 2, row2)
        score(2, 1, 2, row0 + near0 + near1 + row2)

        half = lax.broadcasted_iota(jnp.int32, (8, 128), 1) < 64
        for rel in range(RING):
            for dy in range(RING):
                s = jnp.where(sub < 4, total[rel, 0, dy], total[rel, 1, dy])
                s = s[:, :128] + s[:, 128:]
                sums[rel, (y + RING - dy) % RING] = s + pltpu.roll(s, 64, 1)
        temp = temp_ref[...]
        logits = []
        for rel in range(RING):
            s = jnp.concatenate([jnp.where(half, sums[rel, i], sums[rel, i + 1]) for i in (0, 2)], axis=1)
            s = s + pltpu.roll(s, n_q, 1)
            s = s + pltpu.roll(s, 2 * n_q, 1)
            logits.append(s / temp)
        peak = jnp.maximum(jnp.maximum(logits[0], logits[1]), jnp.maximum(logits[2], logits[3]))
        peak = jnp.max(peak, axis=0, keepdims=True)
        mass = sum(jnp.exp(g - peak) for g in logits)
        part = peak + jnp.log(jnp.sum(mass, axis=0, keepdims=True))
        lanes = lax.broadcasted_iota(jnp.int32, (8, plane), 1)
        is_own = (sub == lanes % n_q) & (lanes // SLOT == y * RING + x) & (lanes % SLOT >= SLOT - n_q)
        own = jnp.sum(jnp.where(is_own, logits[0], 0.0), axis=0, keepdims=True)
        own_sum = jnp.sum(own, axis=1, keepdims=True)
        slot = lax.broadcasted_iota(jnp.int32, (1, 128), 1) % SLOT

        def fold(row):
            return jnp.where(slot >= 12, row[:, :128], pltpu.roll(row[:, 128:], 128 - n_q, 1))

        row = jnp.where(slot >= 8, fold(part), own_sum)
        own = fold(own)
        here = core * RING ** 3 + me
        pieces[here] = row

        def tell(across, dz, dy, dx):
            other = at(dz, dy, dx) | {'data2': 1 - core if across else core}
            return pltpu.make_async_remote_copy(
                src_ref=pieces.at[here], dst_ref=pieces.at[here], send_sem=rsend, recv_sem=rrecv,
                device_id=other)

        rest = [(a, i, j, k) for a in range(2) for i in range(RING) for j in range(RING) for k in range(RING)]
        for a, i, j, k in sorted(rest[1:], key=lambda o: (-far(*o[1:]), -o[0])):
            tell(a, i, j, k).start()
        everyone = pieces.at[pl.ds(0, n_dev - 1)]
        pltpu.make_async_copy(everyone, everyone, rrecv).wait()
        ls = pieces[...].reshape(2 * RING, RING * RING, 128)
        peak = jnp.max(ls, axis=1, keepdims=True)
        mass = jnp.sum(jnp.exp(ls - peak), axis=1)
        whole = peak.reshape(2 * RING, 128) + jnp.log(mass)
        slot = lax.broadcasted_iota(jnp.int32, whole.shape, 1) % SLOT
        answer = jnp.where(slot >= 8, whole, 0.0)
        lane = lax.broadcasted_iota(jnp.int32, whole.shape, 1)
        answer = answer - jnp.where(lane == 0, jnp.sum(ls, axis=1), 0.0)
        answer = jnp.sum(jnp.sum(answer, axis=1, keepdims=True), axis=0, keepdims=True)
        group = lax.broadcasted_iota(jnp.int32, whole.shape, 0)
        losses = jnp.sum(jnp.where(group == core * RING + z, whole, 0.0), axis=0, keepdims=True)
        losses = losses - own
        spot = (y * RING + x) % 8 * SLOT + jnp.where(y >= 2, 8, 12)
        losses = pltpu.roll(jnp.broadcast_to(losses, (8, 128)), (128 - spot) % 128, 1)
        out_ref[0:1] = losses[0:1]
        out_ref[1:2] = jnp.broadcast_to(answer / (n_dev * n_q), (1, 128))

        pltpu.make_async_copy(sent, sent, send).wait()
        pltpu.make_async_copy(everyone, everyone, rsend).wait()

    return kernel


def hand_over(found_ref, loss_ref, mean_ref):
    loss_ref[...] = found_ref[0:1, :loss_ref.shape[1]]
    mean_ref[...] = found_ref[1:2, 0:1]


def solution(mesh):
    row_spec = P(('replica', 'data2', 'data'))
    tok_spec = P(('replica', 'data2', 'data'), None, None)
    mask_spec = P(('replica', 'data2', 'data'), None)

    def local_step(query_hidden, doc_hidden, w_proj, query_mask, doc_mask, temperature):
        n_q, qlen, hidden = query_hidden.shape
        n_docs, dlen, _ = doc_hidden.shape
        proj = w_proj.shape[1]
        chunks = n_q * qlen // SLOT
        sent_rows = (RING * (RING - 1) - 1 + RING) * n_q * qlen + 7 * n_docs * dlen
        dma = pltpu.SemaphoreType.DMA
        found = pl.pallas_call(
            make_kernel(n_docs, dlen, n_q, qlen),
            out_shape=pltpu.VMEM((2, 128), jnp.float32),
            in_specs=[pl.BlockSpec(memory_space=pl.ANY)] * 6,
            out_specs=pl.BlockSpec(memory_space=pltpu.VMEM),
            scratch_shapes=[
                pltpu.VMEM(query_hidden.shape, jnp.bfloat16),
                pltpu.VMEM((dlen, n_docs, hidden), jnp.bfloat16),
                pltpu.VMEM(w_proj.shape, jnp.bfloat16),
                pltpu.VMEM(query_mask.shape, jnp.int32),
                pltpu.VMEM(doc_mask.shape, jnp.int32),
                pltpu.VMEM((1, 1), jnp.float32),
                pltpu.VMEM((chunks, RING, RING, SLOT, proj), jnp.bfloat16),
                pltpu.VMEM((RING, 2, n_docs * dlen, proj), jnp.bfloat16),
                pltpu.VMEM((RING, RING, 8, 128), jnp.float32),
                pltpu.VMEM((2 * RING ** 3, 1, 128), jnp.float32),
                pltpu.VMEM((sent_rows, proj), jnp.bfloat16),
                dma((6,)), dma, dma((13,)), dma, dma,
                pltpu.SemaphoreType.REGULAR,
            ],
            compiler_params=pltpu.CompilerParams(collective_id=0, has_side_effects=True),
        )(query_hidden, jnp.transpose(doc_hidden, (1, 0, 2)), w_proj, query_mask, doc_mask,
          temperature.reshape(1, 1))
        losses, mean = pl.pallas_call(
            hand_over,
            out_shape=(jax.ShapeDtypeStruct((1, n_q), jnp.float32),
                       jax.ShapeDtypeStruct((1, 1), jnp.float32)),
            in_specs=[pl.BlockSpec(memory_space=pltpu.VMEM)],
            out_specs=(pl.BlockSpec(memory_space=pltpu.VMEM),) * 2,
            compiler_params=pltpu.CompilerParams(vmem_limit_bytes=2 ** 20))(found)
        return losses.reshape(n_q), mean.reshape(1)

    return jax.shard_map(local_step, mesh=mesh,
                         in_specs=(tok_spec, tok_spec, P(None, None), mask_spec, mask_spec, P()),
                         out_specs=(row_spec, P('replica')), check_vma=False)
```

```python
import jax
import jax.numpy as jnp
from jax import lax
from jax.experimental import pallas as pl
from jax.experimental.pallas import tpu as pltpu
from jax.sharding import PartitionSpec as P

RING = 4
SLOT = 16
OTHERS = (1, 2, 3)
ROW0, NEAR0, NEAR1, ROW2, SIDE0, SIDE1, PASSED, SWAP0, SWAP1, SWAP2 = 0, (1, 2), 3, 4, (5, 6, 13, 14), 7, 8, 9, (10, 11), 12


def unit_rows(hidden, w):
    projected = jnp.dot(hidden, w, preferred_element_type=jnp.float32)
    norm_len = jnp.sqrt(jnp.sum(projected * projected, axis=-1, keepdims=True))
    return projected / jnp.maximum(norm_len, 1e-12)


def as_column(row_mask, rows):
    r = lax.broadcasted_iota(jnp.int32, (rows, rows), 0)
    c = lax.broadcasted_iota(jnp.int32, (rows, rows), 1)
    return jnp.sum(jnp.where(r == c, row_mask, 0.0), axis=1, keepdims=True)


def far(*offsets):
    return sum(min(o, RING - o) for o in offsets)


def make_kernel(n_docs, dlen, n_q, qlen):
    doc_rows = n_docs * dlen
    head = doc_rows // 2 // 16 * 16 + 16
    cuts = (0, head // 32 * 16 + 16, head, head + (doc_rows - head) // 32 * 16, doc_rows)
    parts = (pl.ds(0, head), pl.ds(head, doc_rows - head), pl.ds(0, doc_rows))
    parts += tuple(pl.ds(a, b - a) for a, b in zip(cuts, cuts[1:]))
    chunks = n_q * qlen // SLOT
    tiles = chunks // RING
    rounds = 4
    plane = RING * RING * SLOT
    n_dev = 2 * RING ** 3

    def kernel(qh_hbm, dh_hbm, w_hbm, qm_hbm, dm_hbm, temp_hbm, out_ref,
               qh, dh, w, qm_ref, dm_ref, temp_ref, qbuf, pbuf, sums, pieces,
               sent, q_rows_ref, load_sem, send, recv, rsend, rrecv, ready):
        loads = [pltpu.make_async_copy(src, dst, load_sem.at[i]) for i, (src, dst) in enumerate((
            (w_hbm, w), (qh_hbm, qh), (qm_hbm, qm_ref), (dm_hbm, dm_ref), (dh_hbm, dh),
            (temp_hbm, temp_ref)))]
        for load in loads:
            load.start()

        core = lax.axis_index('data2')
        me = lax.axis_index('data')
        z, y, x = me // (RING * RING), (me // RING) % RING, me % RING

        zs = [(z + i) % RING * RING * RING for i in range(RING)]
        ys = [(y + i) % RING * RING for i in range(RING)]
        xs = [(x + i) % RING for i in range(RING)]

        def at(dz, dy, dx):
            return {'data': zs[dz] + ys[dy] + xs[dx]}

        sibling = {'data2': 1 - core}
        up, down = at(1, 0, 0), at(RING - 1, 0, 0)
        barrier = pltpu.get_barrier_semaphore()
        mates = [(dy, dx) for dy in (0, 1, 3) for dx in range(RING) if dy or dx]
        mates.sort(key=lambda m: (far(m[0]), -far(m[1])))
        near = [at(0, 0, o) for o in OTHERS] + [at(0, o, 0) for o in OTHERS] + [sibling]
        near += [at(o, 0, 0) for o in OTHERS] + [at(o, 0, 0) | sibling for o in OTHERS]
        for device in near:
            pl.semaphore_signal(barrier, inc=1, device_id=device)

        q_rows = n_q * qlen
        r = lax.broadcasted_iota(jnp.int32, (doc_rows, dlen), 0)
        c = lax.broadcasted_iota(jnp.int32, (doc_rows, dlen), 1)
        spread = jnp.where(r // n_docs == c, 1.0, 0.0).astype(jnp.bfloat16)
        loads[2].wait()
        qm = qm_ref[...].astype(jnp.float32)
        q_keep = jnp.concatenate([as_column(qm[i:i + 1], qlen) for i in range(n_q)], axis=0)

        loads[0].wait()
        loads[1].wait()
        w_val = w[...]
        q_unit = unit_rows(qh[...].reshape(q_rows, qh.shape[2]), w_val)
        q_rows_ref[...] = jnp.where(q_keep > 0, q_unit, 0.0)
        for k in range(chunks):
            block = [q_rows_ref[pl.ds(k * (SLOT // n_q) + t, n_q, stride=qlen)] for t in range(SLOT // n_q)]
            qbuf[k, y, x] = jnp.concatenate(block, axis=0).astype(jnp.bfloat16)

        def query_copy(mate, rnd):
            ref = qbuf.at[pl.ds(rnd * (chunks // rounds), chunks // rounds), y, x]
            dy, t = mate[0], rnd * tiles // rounds
            sem = ROW0 if dy == 0 else NEAR0[t] if t == dy // 2 else NEAR1
            return pltpu.make_async_remote_copy(
                src_ref=ref, dst_ref=ref, send_sem=send, recv_sem=recv.at[sem], device_id=at(0, *mate))

        def arrived(sem, ref):
            pltpu.make_async_copy(ref, ref, recv.at[sem]).wait()

        def row_part(dy, t):
            return qbuf.at[pl.ds(t * RING, RING), (y + RING - dy) % RING]

        def row_copy(dy):
            ref = row_part(dy, 0 if dy == 1 else 1)
            return pltpu.make_async_remote_copy(
                src_ref=ref, dst_ref=ref, send_sem=send, recv_sem=recv.at[ROW2],
                device_id=at(0, dy, 0))

        loads[3].wait()
        loads[4].wait()
        dm = dm_ref[...].astype(jnp.float32)
        lane = lax.broadcasted_iota(jnp.int32, dm.shape, 1)
        first = jnp.min(jnp.where(dm > 0, lane, dlen), axis=1, keepdims=True)
        r = lax.broadcasted_iota(jnp.int32, (n_docs, doc_rows), 1)
        d = lax.broadcasted_iota(jnp.int32, (n_docs, doc_rows), 0)
        pick = jnp.where(r == first * n_docs + d, 1.0, 0.0).astype(jnp.bfloat16)
        keep = lax.dot_general(spread, dm.astype(jnp.bfloat16), (((1,), (1,)), ((), ())),
                               preferred_element_type=jnp.float32)
        r = lax.broadcasted_iota(jnp.int32, keep.shape, 0)
        c = lax.broadcasted_iota(jnp.int32, keep.shape, 1)
        keep = jnp.sum(jnp.where(r % n_docs == c, keep, 0.0), axis=1, keepdims=True)
        cut = dlen // 5
        unit = jnp.concatenate([
            unit_rows(dh[i:i + cut].reshape(cut * n_docs, dh.shape[2]), w[...])
            for i in range(0, dlen, cut)], axis=0)
        unit = jnp.where(keep > 0, unit, 0.0).astype(jnp.bfloat16)
        valid = jnp.dot(pick, unit, preferred_element_type=jnp.float32)
        valid = jnp.concatenate([valid, valid], axis=0)
        valid = jnp.broadcast_to(valid[None], (doc_rows // 8, 8, valid.shape[1]))
        filled = jnp.where(keep > 0, unit.astype(jnp.float32), valid.reshape(doc_rows, valid.shape[2]))
        pbuf[z, core] = filled.astype(jnp.bfloat16)

        def doc_part(rel, h):
            return pbuf.at[(z + rel) % RING, core, parts[h]]

        def swap_copy(rel, h):
            ref = doc_part(rel, h)
            sem = SWAP0 if rel == 0 else SWAP2 if rel == 2 else SWAP1[rel // 2 == h]
            return pltpu.make_async_remote_copy(
                src_ref=ref, dst_ref=ref, send_sem=send, recv_sem=recv.at[sem], device_id=sibling)

        def z_copy(way, h):
            ref = doc_part(0, h)
            sem = SIDE1 if h < 2 else SIDE0[h - 3]
            return pltpu.make_async_remote_copy(
                src_ref=ref, dst_ref=ref, send_sem=send, recv_sem=recv.at[sem],
                device_id=down if way else up)

        def pass_copy(way, i):
            ref = doc_part(1 if way else RING - 1, 3 + 2 * way + i)
            return pltpu.make_async_remote_copy(
                src_ref=ref, dst_ref=ref, send_sem=send, recv_sem=recv.at[PASSED],
                device_id=down if way else up)

        loads[5].wait()
        pl.semaphore_wait(barrier, len(near))
        for off in OTHERS:
            pl.semaphore_signal(ready, inc=1, device_id=at(0, 0, off))
        for i in range(3):
            for way in range(2):
                z_copy(way, 1 - way if i == 2 else 3 + 2 * way + i).start()
        for rnd in range(rounds):
            for mate in mates:
                if 0 in mate:
                    query_copy(mate, rnd).start()
        swap_copy(0, 2).start()
        pl.semaphore_wait(ready, 3)
        for i in range(tiles):
            for rnd in range(rounds // tiles):
                for mate in mates:
                    if 0 not in mate:
                        t = i if mate[0] == 1 else 1 - i
                        query_copy(mate, t * (rounds // tiles) + rnd).start()

        sub = lax.broadcasted_iota(jnp.int32, (8, plane), 0)
        found, total = {}, {}

        def score(rel, swapped, part, spots):
            docs = pbuf[(z + rel) % RING, 1 - core if swapped else core, parts[part]]
            for dy, t in spots:
                q_tile = row_part(dy, t)[...].reshape(plane, qbuf.shape[-1])
                sim = lax.dot_general(docs, q_tile, (((1,), (1,)), ((), ())),
                                      preferred_element_type=jnp.float32)
                best = jnp.max(sim.reshape(docs.shape[0] // 8, 8, plane), axis=0)
                tile, key = (rel, swapped, dy, t), (rel, swapped, dy)
                if part < 2 and tile not in found:
                    found[tile] = best
                    continue
                if part < 2:
                    best = jnp.maximum(best, found[tile])
                best = jnp.maximum(best, pltpu.roll(best, 4, 0))
                total[key] = total[key] + best if key in total else best

        sides, row0 = ((0, 3), (1, 1)), ((0, 0), (0, 1))
        near0, near1, row2 = ((1, 0), (3, 1)), ((1, 1), (3, 0)), ((2, 0), (2, 1))
        docs_ref, row_ref = pbuf.at[z, core], qbuf.at[:, y]
        arrived(ROW0, row_ref.at[:, pl.ds(0, RING - 1)])
        arrived(SWAP0, docs_ref)
        score(0, 0, 2, row0)
        score(0, 1, 2, row0)
        for i in range(2):
            for way in range(2):
                z_copy(way, 3 + 2 * way + i).wait_recv()
                pass_copy(way, i).start()
                if i:
                    swap_copy(1 if way else 3, way).start()
        for way, rel in sides:
            score(rel, 0, way, row0)
        arrived(SIDE1, docs_ref)
        for way in range(2):
            swap_copy(1 if way else 3, 1 - way).start()
        arrived(SWAP1[0], docs_ref)
        arrived(NEAR0[0], row_part(1, 0))
        row_copy(1).start()
        arrived(NEAR0[1], row_part(3, 1))
        row_copy(3).start()
        for way, rel in sides:
            score(rel, 0, 1 - way, row0)
            score(rel, 1, way, row0)
        for spots in (near0, near1):
            if spots is near1:
                arrived(NEAR1, row_ref)
            score(0, 0, 2, spots)
            score(0, 1, 2, spots)
            for way, rel in sides:
                score(rel, 0, way, spots)
                score(rel, 1, way, spots)
                score(rel, 0, 1 - way, spots)
        arrived(PASSED, docs_ref)
        for way in range(2):
            swap_copy(2, way).start()
        arrived(SWAP1[1], docs_ref)
        for way, rel in sides:
            score(rel, 1, 1 - way, row0 + near0 + near1)
        score(2, 0, 2, row0 + near0 + near1)
        arrived(ROW2, row_ref)
        arrived(SWAP2, docs_ref)
        score(0, 0, 2, row2)
        score(0, 1, 2, row2)
        for way, rel in sides:
            for side in range(2):
                score(rel, side, way, row2)
                score(rel, side, 1 - way, row2)
        score(2, 0, 2, row2)
        score(2, 1, 2, row0 + near0 + near1 + row2)

        half = lax.broadcasted_iota(jnp.int32, (8, 128), 1) < 64
        for rel in range(RING):
            for dy in range(RING):
                s = jnp.where(sub < 4, total[rel, 0, dy], total[rel, 1, dy])
                s = s[:, :128] + s[:, 128:]
                sums[rel, (y + RING - dy) % RING] = s + pltpu.roll(s, 64, 1)
        temp = temp_ref[...]
        logits = []
        for rel in range(RING):
            s = jnp.concatenate([jnp.where(half, sums[rel, i], sums[rel, i + 1]) for i in (0, 2)], axis=1)
            s = s + pltpu.roll(s, n_q, 1)
            s = s + pltpu.roll(s, 2 * n_q, 1)
            logits.append(s / temp)
        peak = jnp.maximum(jnp.maximum(logits[0], logits[1]), jnp.maximum(logits[2], logits[3]))
        peak = jnp.max(peak, axis=0, keepdims=True)
        mass = sum(jnp.exp(g - peak) for g in logits)
        part = peak + jnp.log(jnp.sum(mass, axis=0, keepdims=True))
        lanes = lax.broadcasted_iota(jnp.int32, (8, plane), 1)
        is_own = (sub == lanes % n_q) & (lanes // SLOT == y * RING + x) & (lanes % SLOT >= SLOT - n_q)
        own = jnp.sum(jnp.where(is_own, logits[0], 0.0), axis=0, keepdims=True)
        own_sum = jnp.sum(own, axis=1, keepdims=True)
        slot = lax.broadcasted_iota(jnp.int32, (1, 128), 1) % SLOT

        def fold(row):
            return jnp.where(slot >= 12, row[:, :128], pltpu.roll(row[:, 128:], 128 - n_q, 1))

        row = jnp.where(slot >= 8, fold(part), own_sum)
        own = fold(own)
        here = core * RING ** 3 + me
        pieces[here] = row

        def tell(across, dz, dy, dx):
            other = at(dz, dy, dx) | {'data2': 1 - core if across else core}
            return pltpu.make_async_remote_copy(
                src_ref=pieces.at[here], dst_ref=pieces.at[here], send_sem=rsend, recv_sem=rrecv,
                device_id=other)

        rest = [(a, i, j, k) for a in range(2) for i in range(RING) for j in range(RING) for k in range(RING)]
        for a, i, j, k in sorted(rest[1:], key=lambda o: (-far(*o[1:]), -o[0])):
            tell(a, i, j, k).start()
        everyone = pieces.at[pl.ds(0, n_dev - 1)]
        pltpu.make_async_copy(everyone, everyone, rrecv).wait()
        ls = pieces[...].reshape(2 * RING, RING * RING, 128)
        peak = jnp.max(ls, axis=1, keepdims=True)
        mass = jnp.sum(jnp.exp(ls - peak), axis=1)
        whole = peak.reshape(2 * RING, 128) + jnp.log(mass)
        slot = lax.broadcasted_iota(jnp.int32, whole.shape, 1) % SLOT
        answer = jnp.where(slot >= 8, whole, 0.0)
        lane = lax.broadcasted_iota(jnp.int32, whole.shape, 1)
        answer = answer - jnp.where(lane == 0, jnp.sum(ls, axis=1), 0.0)
        answer = jnp.sum(jnp.sum(answer, axis=1, keepdims=True), axis=0, keepdims=True)
        group = lax.broadcasted_iota(jnp.int32, whole.shape, 0)
        losses = jnp.sum(jnp.where(group == core * RING + z, whole, 0.0), axis=0, keepdims=True)
        losses = losses - own
        spot = (y * RING + x) % 8 * SLOT + jnp.where(y >= 2, 8, 12)
        losses = pltpu.roll(jnp.broadcast_to(losses, (8, 128)), (128 - spot) % 128, 1)
        out_ref[0:1] = losses[0:1]
        out_ref[1:2] = jnp.broadcast_to(answer / (n_dev * n_q), (1, 128))

        pltpu.make_async_copy(sent, sent, send).wait()
        pltpu.make_async_copy(everyone, everyone, rsend).wait()

    return kernel


def hand_over(found_ref, loss_ref, mean_ref):
    loss_ref[...] = found_ref[0:1, :loss_ref.shape[1]]
    mean_ref[...] = found_ref[1:2, 0:1]


def solution(mesh):
    row_spec = P(('replica', 'data2', 'data'))
    tok_spec = P(('replica', 'data2', 'data'), None, None)
    mask_spec = P(('replica', 'data2', 'data'), None)

    def local_step(query_hidden, doc_hidden, w_proj, query_mask, doc_mask, temperature):
        n_q, qlen, hidden = query_hidden.shape
        n_docs, dlen, _ = doc_hidden.shape
        proj = w_proj.shape[1]
        chunks = n_q * qlen // SLOT
        sent_rows = (RING * (RING - 1) - 1 + RING) * n_q * qlen + 7 * n_docs * dlen
        dma = pltpu.SemaphoreType.DMA
        found = pl.pallas_call(
            make_kernel(n_docs, dlen, n_q, qlen),
            out_shape=pltpu.VMEM((2, 128), jnp.float32),
            in_specs=[pl.BlockSpec(memory_space=pl.ANY)] * 6,
            out_specs=pl.BlockSpec(memory_space=pltpu.VMEM),
            scratch_shapes=[
                pltpu.VMEM(query_hidden.shape, jnp.bfloat16),
                pltpu.VMEM((dlen, n_docs, hidden), jnp.bfloat16),
                pltpu.VMEM(w_proj.shape, jnp.bfloat16),
                pltpu.VMEM(query_mask.shape, jnp.int32),
                pltpu.VMEM(doc_mask.shape, jnp.int32),
                pltpu.VMEM((1, 1), jnp.float32),
                pltpu.VMEM((chunks, RING, RING, SLOT, proj), jnp.bfloat16),
                pltpu.VMEM((RING, 2, n_docs * dlen, proj), jnp.bfloat16),
                pltpu.VMEM((RING, RING, 8, 128), jnp.float32),
                pltpu.VMEM((2 * RING ** 3, 1, 128), jnp.float32),
                pltpu.VMEM((sent_rows, proj), jnp.bfloat16),
                pltpu.VMEM((n_q * qlen, proj), jnp.float32),
                dma((6,)), dma, dma((15,)), dma, dma,
                pltpu.SemaphoreType.REGULAR,
            ],
            compiler_params=pltpu.CompilerParams(collective_id=0, has_side_effects=True),
        )(query_hidden, jnp.transpose(doc_hidden, (1, 0, 2)), w_proj, query_mask, doc_mask,
          temperature.reshape(1, 1))
        losses, mean = pl.pallas_call(
            hand_over,
            out_shape=(jax.ShapeDtypeStruct((1, n_q), jnp.float32),
                       jax.ShapeDtypeStruct((1, 1), jnp.float32)),
            in_specs=[pl.BlockSpec(memory_space=pltpu.VMEM)],
            out_specs=(pl.BlockSpec(memory_space=pltpu.VMEM),) * 2,
            compiler_params=pltpu.CompilerParams(vmem_limit_bytes=2 ** 20))(found)
        return losses.reshape(n_q), mean.reshape(1)

    return jax.shard_map(local_step, mesh=mesh,
                         in_specs=(tok_spec, tok_spec, P(None, None), mask_spec, mask_spec, P()),
                         out_specs=(row_spec, P('replica')), check_vma=False)
```

```python
import jax
import jax.numpy as jnp
from jax import lax
from jax.experimental import pallas as pl
from jax.experimental.pallas import tpu as pltpu
from jax.sharding import PartitionSpec as P

RING = 4
SLOT = 16
OTHERS = (1, 2, 3)
ROW0, NEAR0, NEAR1, ROW2, SIDE0, SIDE1, PASSED, SWAP0, SWAP1, SWAP2 = 0, (1, 2), 3, 4, (5, 6, 13, 14), 7, 8, 9, (10, 11), 12


def unit_rows(hidden, w):
    projected = jnp.dot(hidden, w, preferred_element_type=jnp.float32)
    norm_len = jnp.sqrt(jnp.sum(projected * projected, axis=-1, keepdims=True))
    return projected / jnp.maximum(norm_len, 1e-12)


def as_column(row_mask, rows):
    r = lax.broadcasted_iota(jnp.int32, (rows, rows), 0)
    c = lax.broadcasted_iota(jnp.int32, (rows, rows), 1)
    return jnp.sum(jnp.where(r == c, row_mask, 0.0), axis=1, keepdims=True)


def far(*offsets):
    return sum(min(o, RING - o) for o in offsets)


def make_kernel(n_docs, dlen, n_q, qlen):
    doc_rows = n_docs * dlen
    head = doc_rows // 2 // 16 * 16 + 16
    cuts = (0, head // 32 * 16 + 16, head, head + (doc_rows - head) // 32 * 16, doc_rows)
    parts = (pl.ds(0, head), pl.ds(head, doc_rows - head), pl.ds(0, doc_rows))
    parts += tuple(pl.ds(a, b - a) for a, b in zip(cuts, cuts[1:]))
    chunks = n_q * qlen // SLOT
    tiles = chunks // RING
    rounds = 4
    plane = RING * RING * SLOT
    n_dev = 2 * RING ** 3

    def kernel(qh_hbm, dh_hbm, w_hbm, qm_hbm, dm_hbm, temp_hbm, out_ref,
               qh, dh, w, qm_ref, dm_ref, temp_ref, qbuf, pbuf, sums, pieces,
               sent, q_rows_ref, load_sem, send, recv, rsend, rrecv, ready):
        loads = [pltpu.make_async_copy(src, dst, load_sem.at[i]) for i, (src, dst) in enumerate((
            (w_hbm, w), (qh_hbm, qh), (qm_hbm, qm_ref), (dm_hbm, dm_ref), (dh_hbm.at[pl.ds(0, 108)], dh.at[pl.ds(0, 108)]),
            (temp_hbm, temp_ref), (dh_hbm.at[pl.ds(108, 72)], dh.at[pl.ds(108, 72)])))]
        for i, load in enumerate(loads):
            load.start(priority=1 if i in (4, 6) else 0)

        core = lax.axis_index('data2')
        me = lax.axis_index('data')
        z, y, x = me // (RING * RING), (me // RING) % RING, me % RING

        zs = [(z + i) % RING * RING * RING for i in range(RING)]
        ys = [(y + i) % RING * RING for i in range(RING)]
        xs = [(x + i) % RING for i in range(RING)]

        def at(dz, dy, dx):
            return {'data': zs[dz] + ys[dy] + xs[dx]}

        sibling = {'data2': 1 - core}
        up, down = at(1, 0, 0), at(RING - 1, 0, 0)
        barrier = pltpu.get_barrier_semaphore()
        mates = [(dy, dx) for dy in (0, 1, 3) for dx in range(RING) if dy or dx]
        mates.sort(key=lambda m: (far(m[0]), -far(m[1])))
        near = [at(0, 0, o) for o in OTHERS] + [at(0, o, 0) for o in OTHERS] + [sibling]
        near += [at(o, 0, 0) for o in OTHERS] + [at(o, 0, 0) | sibling for o in OTHERS]
        for device in near:
            pl.semaphore_signal(barrier, inc=1, device_id=device)

        q_rows = n_q * qlen
        r = lax.broadcasted_iota(jnp.int32, (doc_rows, dlen), 0)
        c = lax.broadcasted_iota(jnp.int32, (doc_rows, dlen), 1)
        spread = jnp.where(r // n_docs == c, 1.0, 0.0).astype(jnp.bfloat16)
        loads[2].wait()
        qm = qm_ref[...].astype(jnp.float32)
        q_keep = jnp.concatenate([as_column(qm[i:i + 1], qlen) for i in range(n_q)], axis=0)

        loads[0].wait()
        loads[1].wait()
        w_val = w[...]
        q_unit = unit_rows(qh[...].reshape(q_rows, qh.shape[2]), w_val)
        q_rows_ref[...] = jnp.where(q_keep > 0, q_unit, 0.0)
        for k in range(chunks):
            block = [q_rows_ref[pl.ds(k * (SLOT // n_q) + t, n_q, stride=qlen)] for t in range(SLOT // n_q)]
            qbuf[k, y, x] = jnp.concatenate(block, axis=0).astype(jnp.bfloat16)

        def query_copy(mate, rnd):
            ref = qbuf.at[pl.ds(rnd * (chunks // rounds), chunks // rounds), y, x]
            dy, t = mate[0], rnd * tiles // rounds
            sem = ROW0 if dy == 0 else NEAR0[t] if t == dy // 2 else NEAR1
            return pltpu.make_async_remote_copy(
                src_ref=ref, dst_ref=ref, send_sem=send, recv_sem=recv.at[sem], device_id=at(0, *mate))

        def arrived(sem, ref):
            pltpu.make_async_copy(ref, ref, recv.at[sem]).wait()

        def row_part(dy, t):
            return qbuf.at[pl.ds(t * RING, RING), (y + RING - dy) % RING]

        def row_copy(dy):
            ref = row_part(dy, 0 if dy == 1 else 1)
            return pltpu.make_async_remote_copy(
                src_ref=ref, dst_ref=ref, send_sem=send, recv_sem=recv.at[ROW2],
                device_id=at(0, dy, 0))

        loads[3].wait()
        loads[4].wait()
        loads[6].wait()
        dm = dm_ref[...].astype(jnp.float32)
        lane = lax.broadcasted_iota(jnp.int32, dm.shape, 1)
        first = jnp.min(jnp.where(dm > 0, lane, dlen), axis=1, keepdims=True)
        r = lax.broadcasted_iota(jnp.int32, (n_docs, doc_rows), 1)
        d = lax.broadcasted_iota(jnp.int32, (n_docs, doc_rows), 0)
        pick = jnp.where(r == first * n_docs + d, 1.0, 0.0).astype(jnp.bfloat16)
        keep = lax.dot_general(spread, dm.astype(jnp.bfloat16), (((1,), (1,)), ((), ())),
                               preferred_element_type=jnp.float32)
        r = lax.broadcasted_iota(jnp.int32, keep.shape, 0)
        c = lax.broadcasted_iota(jnp.int32, keep.shape, 1)
        keep = jnp.sum(jnp.where(r % n_docs == c, keep, 0.0), axis=1, keepdims=True)
        cut = dlen // 5
        unit = jnp.concatenate([
            unit_rows(dh[i:i + cut].reshape(cut * n_docs, dh.shape[2]), w[...])
            for i in range(0, dlen, cut)], axis=0)
        unit = jnp.where(keep > 0, unit, 0.0).astype(jnp.bfloat16)
        valid = jnp.dot(pick, unit, preferred_element_type=jnp.float32)
        valid = jnp.concatenate([valid, valid], axis=0)
        valid = jnp.broadcast_to(valid[None], (doc_rows // 8, 8, valid.shape[1]))
        filled = jnp.where(keep > 0, unit.astype(jnp.float32), valid.reshape(doc_rows, valid.shape[2]))
        pbuf[z, core] = filled.astype(jnp.bfloat16)

        def doc_part(rel, h):
            return pbuf.at[(z + rel) % RING, core, parts[h]]

        def swap_copy(rel, h):
            ref = doc_part(rel, h)
            sem = SWAP0 if rel == 0 else SWAP2 if rel == 2 else SWAP1[rel // 2 == h]
            return pltpu.make_async_remote_copy(
                src_ref=ref, dst_ref=ref, send_sem=send, recv_sem=recv.at[sem], device_id=sibling)

        def z_copy(way, h):
            ref = doc_part(0, h)
            sem = SIDE1 if h < 2 else SIDE0[h - 3]
            return pltpu.make_async_remote_copy(
                src_ref=ref, dst_ref=ref, send_sem=send, recv_sem=recv.at[sem],
                device_id=down if way else up)

        def pass_copy(way, i):
            ref = doc_part(1 if way else RING - 1, 3 + 2 * way + i)
            return pltpu.make_async_remote_copy(
                src_ref=ref, dst_ref=ref, send_sem=send, recv_sem=recv.at[PASSED],
                device_id=down if way else up)

        loads[5].wait()
        pl.semaphore_wait(barrier, len(near))
        for off in OTHERS:
            pl.semaphore_signal(ready, inc=1, device_id=at(0, 0, off))
        for i in range(3):
            for way in range(2):
                z_copy(way, 1 - way if i == 2 else 3 + 2 * way + i).start()
        for rnd in range(rounds):
            for mate in mates:
                if 0 in mate:
                    query_copy(mate, rnd).start()
        swap_copy(0, 2).start()
        pl.semaphore_wait(ready, 3)
        for i in range(tiles):
            for rnd in range(rounds // tiles):
                for mate in mates:
                    if 0 not in mate:
                        t = i if mate[0] == 1 else 1 - i
                        query_copy(mate, t * (rounds // tiles) + rnd).start()

        sub = lax.broadcasted_iota(jnp.int32, (8, plane), 0)
        found, total = {}, {}

        def score(rel, swapped, part, spots):
            docs = pbuf[(z + rel) % RING, 1 - core if swapped else core, parts[part]]
            for dy, t in spots:
                q_tile = row_part(dy, t)[...].reshape(plane, qbuf.shape[-1])
                sim = lax.dot_general(docs, q_tile, (((1,), (1,)), ((), ())),
                                      preferred_element_type=jnp.float32)
                best = jnp.max(sim.reshape(docs.shape[0] // 8, 8, plane), axis=0)
                tile, key = (rel, swapped, dy, t), (rel, swapped, dy)
                if part < 2 and tile not in found:
                    found[tile] = best
                    continue
                if part < 2:
                    best = jnp.maximum(best, found[tile])
                best = jnp.maximum(best, pltpu.roll(best, 4, 0))
                total[key] = total[key] + best if key in total else best

        sides, row0 = ((0, 3), (1, 1)), ((0, 0), (0, 1))
        near0, near1, row2 = ((1, 0), (3, 1)), ((1, 1), (3, 0)), ((2, 0), (2, 1))
        docs_ref, row_ref = pbuf.at[z, core], qbuf.at[:, y]
        arrived(ROW0, row_ref.at[:, pl.ds(0, RING - 1)])
        arrived(SWAP0, docs_ref)
        score(0, 0, 2, row0)
        score(0, 1, 2, row0)
        for i in range(2):
            for way in range(2):
                z_copy(way, 3 + 2 * way + i).wait_recv()
                pass_copy(way, i).start()
                if i:
                    swap_copy(1 if way else 3, way).start()
        for way, rel in sides:
            score(rel, 0, way, row0)
        arrived(SIDE1, docs_ref)
        for way in range(2):
            swap_copy(1 if way else 3, 1 - way).start()
        arrived(SWAP1[0], docs_ref)
        arrived(NEAR0[0], row_part(1, 0))
        row_copy(1).start()
        arrived(NEAR0[1], row_part(3, 1))
        row_copy(3).start()
        for way, rel in sides:
            score(rel, 0, 1 - way, row0)
            score(rel, 1, way, row0)
        for spots in (near0, near1):
            if spots is near1:
                arrived(NEAR1, row_ref)
            score(0, 0, 2, spots)
            score(0, 1, 2, spots)
            for way, rel in sides:
                score(rel, 0, way, spots)
                score(rel, 1, way, spots)
                score(rel, 0, 1 - way, spots)
        arrived(PASSED, docs_ref)
        for way in range(2):
            swap_copy(2, way).start()
        arrived(SWAP1[1], docs_ref)
        for way, rel in sides:
            score(rel, 1, 1 - way, row0 + near0 + near1)
        score(2, 0, 2, row0 + near0 + near1)
        arrived(ROW2, row_ref)
        arrived(SWAP2, docs_ref)
        score(0, 0, 2, row2)
        score(0, 1, 2, row2)
        for way, rel in sides:
            for side in range(2):
                score(rel, side, way, row2)
                score(rel, side, 1 - way, row2)
        score(2, 0, 2, row2)
        score(2, 1, 2, row0 + near0 + near1 + row2)

        half = lax.broadcasted_iota(jnp.int32, (8, 128), 1) < 64
        for rel in range(RING):
            for dy in range(RING):
                s = jnp.where(sub < 4, total[rel, 0, dy], total[rel, 1, dy])
                s = s[:, :128] + s[:, 128:]
                sums[rel, (y + RING - dy) % RING] = s + pltpu.roll(s, 64, 1)
        temp = temp_ref[...]
        logits = []
        for rel in range(RING):
            s = jnp.concatenate([jnp.where(half, sums[rel, i], sums[rel, i + 1]) for i in (0, 2)], axis=1)
            s = s + pltpu.roll(s, n_q, 1)
            s = s + pltpu.roll(s, 2 * n_q, 1)
            logits.append(s / temp)
        peak = jnp.maximum(jnp.maximum(logits[0], logits[1]), jnp.maximum(logits[2], logits[3]))
        peak = jnp.max(peak, axis=0, keepdims=True)
        mass = sum(jnp.exp(g - peak) for g in logits)
        part = peak + jnp.log(jnp.sum(mass, axis=0, keepdims=True))
        lanes = lax.broadcasted_iota(jnp.int32, (8, plane), 1)
        is_own = (sub == lanes % n_q) & (lanes // SLOT == y * RING + x) & (lanes % SLOT >= SLOT - n_q)
        own = jnp.sum(jnp.where(is_own, logits[0], 0.0), axis=0, keepdims=True)
        own_sum = jnp.sum(own, axis=1, keepdims=True)
        slot = lax.broadcasted_iota(jnp.int32, (1, 128), 1) % SLOT

        def fold(row):
            return jnp.where(slot >= 12, row[:, :128], pltpu.roll(row[:, 128:], 128 - n_q, 1))

        row = jnp.where(slot >= 8, fold(part), own_sum)
        own = fold(own)
        here = core * RING ** 3 + me
        pieces[here] = row

        def tell(across, dz, dy, dx):
            other = at(dz, dy, dx) | {'data2': 1 - core if across else core}
            return pltpu.make_async_remote_copy(
                src_ref=pieces.at[here], dst_ref=pieces.at[here], send_sem=rsend, recv_sem=rrecv,
                device_id=other)

        rest = [(a, i, j, k) for a in range(2) for i in range(RING) for j in range(RING) for k in range(RING)]
        for a, i, j, k in sorted(rest[1:], key=lambda o: (-far(*o[1:]), -o[0])):
            tell(a, i, j, k).start()
        everyone = pieces.at[pl.ds(0, n_dev - 1)]
        pltpu.make_async_copy(everyone, everyone, rrecv).wait()
        ls = pieces[...].reshape(2 * RING, RING * RING, 128)
        peak = jnp.max(ls, axis=1, keepdims=True)
        mass = jnp.sum(jnp.exp(ls - peak), axis=1)
        whole = peak.reshape(2 * RING, 128) + jnp.log(mass)
        slot = lax.broadcasted_iota(jnp.int32, whole.shape, 1) % SLOT
        answer = jnp.where(slot >= 8, whole, 0.0)
        lane = lax.broadcasted_iota(jnp.int32, whole.shape, 1)
        answer = answer - jnp.where(lane == 0, jnp.sum(ls, axis=1), 0.0)
        answer = jnp.sum(jnp.sum(answer, axis=1, keepdims=True), axis=0, keepdims=True)
        group = lax.broadcasted_iota(jnp.int32, whole.shape, 0)
        losses = jnp.sum(jnp.where(group == core * RING + z, whole, 0.0), axis=0, keepdims=True)
        losses = losses - own
        spot = (y * RING + x) % 8 * SLOT + jnp.where(y >= 2, 8, 12)
        losses = pltpu.roll(jnp.broadcast_to(losses, (8, 128)), (128 - spot) % 128, 1)
        out_ref[0:1] = losses[0:1]
        out_ref[1:2] = jnp.broadcast_to(answer / (n_dev * n_q), (1, 128))

        pltpu.make_async_copy(sent, sent, send).wait()
        pltpu.make_async_copy(everyone, everyone, rsend).wait()

    return kernel


def hand_over(found_ref, loss_ref, mean_ref):
    loss_ref[...] = found_ref[0:1, :loss_ref.shape[1]]
    mean_ref[...] = found_ref[1:2, 0:1]


def solution(mesh):
    row_spec = P(('replica', 'data2', 'data'))
    tok_spec = P(('replica', 'data2', 'data'), None, None)
    mask_spec = P(('replica', 'data2', 'data'), None)

    def local_step(query_hidden, doc_hidden, w_proj, query_mask, doc_mask, temperature):
        n_q, qlen, hidden = query_hidden.shape
        n_docs, dlen, _ = doc_hidden.shape
        proj = w_proj.shape[1]
        chunks = n_q * qlen // SLOT
        sent_rows = (RING * (RING - 1) - 1 + RING) * n_q * qlen + 7 * n_docs * dlen
        dma = pltpu.SemaphoreType.DMA
        found = pl.pallas_call(
            make_kernel(n_docs, dlen, n_q, qlen),
            out_shape=pltpu.VMEM((2, 128), jnp.float32),
            in_specs=[pl.BlockSpec(memory_space=pl.ANY)] * 6,
            out_specs=pl.BlockSpec(memory_space=pltpu.VMEM),
            scratch_shapes=[
                pltpu.VMEM(query_hidden.shape, jnp.bfloat16),
                pltpu.VMEM((dlen, n_docs, hidden), jnp.bfloat16),
                pltpu.VMEM(w_proj.shape, jnp.bfloat16),
                pltpu.VMEM(query_mask.shape, jnp.int32),
                pltpu.VMEM(doc_mask.shape, jnp.int32),
                pltpu.VMEM((1, 1), jnp.float32),
                pltpu.VMEM((chunks, RING, RING, SLOT, proj), jnp.bfloat16),
                pltpu.VMEM((RING, 2, n_docs * dlen, proj), jnp.bfloat16),
                pltpu.VMEM((RING, RING, 8, 128), jnp.float32),
                pltpu.VMEM((2 * RING ** 3, 1, 128), jnp.float32),
                pltpu.VMEM((sent_rows, proj), jnp.bfloat16),
                pltpu.VMEM((n_q * qlen, proj), jnp.float32),
                dma((7,)), dma, dma((15,)), dma, dma,
                pltpu.SemaphoreType.REGULAR,
            ],
            compiler_params=pltpu.CompilerParams(collective_id=0, has_side_effects=True),
        )(query_hidden, jnp.transpose(doc_hidden, (1, 0, 2)), w_proj, query_mask, doc_mask,
          temperature.reshape(1, 1))
        losses, mean = pl.pallas_call(
            hand_over,
            out_shape=(jax.ShapeDtypeStruct((1, n_q), jnp.float32),
                       jax.ShapeDtypeStruct((1, 1), jnp.float32)),
            in_specs=[pl.BlockSpec(memory_space=pltpu.VMEM)],
            out_specs=(pl.BlockSpec(memory_space=pltpu.VMEM),) * 2,
            compiler_params=pltpu.CompilerParams(vmem_limit_bytes=2 ** 20))(found)
        return losses.reshape(n_q), mean.reshape(1)

    return jax.shard_map(local_step, mesh=mesh,
                         in_specs=(tok_spec, tok_spec, P(None, None), mask_spec, mask_spec, P()),
                         out_specs=(row_spec, P('replica')), check_vma=False)
```

```python
import jax
import jax.numpy as jnp
from jax import lax
from jax.experimental import pallas as pl
from jax.experimental.pallas import tpu as pltpu
from jax.sharding import PartitionSpec as P

RING = 4
SLOT = 16
OTHERS = (1, 2, 3)
ROW0, NEAR0, NEAR1, ROW2, SIDE0, SIDE1, PASSED, SWAP0, SWAP1, SWAP2 = 0, (1, 2), 3, 4, (5, 6, 13, 14), 7, 8, 9, (10, 11), 12


def unit_rows(hidden, w):
    projected = jnp.dot(hidden, w, preferred_element_type=jnp.float32)
    norm_len = jnp.sqrt(jnp.sum(projected * projected, axis=-1, keepdims=True))
    return projected / jnp.maximum(norm_len, 1e-12)


def as_column(row_mask, rows):
    r = lax.broadcasted_iota(jnp.int32, (rows, rows), 0)
    c = lax.broadcasted_iota(jnp.int32, (rows, rows), 1)
    return jnp.sum(jnp.where(r == c, row_mask, 0.0), axis=1, keepdims=True)


def far(*offsets):
    return sum(min(o, RING - o) for o in offsets)


def make_kernel(n_docs, dlen, n_q, qlen):
    doc_rows = n_docs * dlen
    head = doc_rows // 2 // 16 * 16 + 16
    cuts = (0, head // 32 * 16 + 16, head, head + (doc_rows - head) // 32 * 16, doc_rows)
    parts = (pl.ds(0, head), pl.ds(head, doc_rows - head), pl.ds(0, doc_rows))
    parts += tuple(pl.ds(a, b - a) for a, b in zip(cuts, cuts[1:]))
    chunks = n_q * qlen // SLOT
    tiles = chunks // RING
    rounds = 4
    plane = RING * RING * SLOT
    n_dev = 2 * RING ** 3

    def kernel(qh_hbm, dh_hbm, w_hbm, qm_hbm, dm_hbm, temp_hbm, out_ref,
               qh, dh, w, qm_ref, dm_ref, temp_ref, qbuf, pbuf, sums, pieces,
               sent, q_rows_ref, load_sem, send, recv, rsend, rrecv, ready):
        loads = [pltpu.make_async_copy(src, dst, load_sem.at[(0, 0, 2, 3, 4, 1, 4)[i]]) for i, (src, dst) in enumerate((
            (w_hbm, w), (qh_hbm, qh), (qm_hbm, qm_ref), (dm_hbm, dm_ref), (dh_hbm.at[pl.ds(0, 108)], dh.at[pl.ds(0, 108)]),
            (temp_hbm, temp_ref), (dh_hbm.at[pl.ds(108, 72)], dh.at[pl.ds(108, 72)])))]
        for i, load in enumerate(loads):
            load.start(priority=1 if i in (4, 6) else 0)

        core = lax.axis_index('data2')
        me = lax.axis_index('data')
        z, y, x = me // (RING * RING), (me // RING) % RING, me % RING

        zs = [(z + i) % RING * RING * RING for i in range(RING)]
        ys = [(y + i) % RING * RING for i in range(RING)]
        xs = [(x + i) % RING for i in range(RING)]

        def at(dz, dy, dx):
            return {'data': zs[dz] + ys[dy] + xs[dx]}

        sibling = {'data2': 1 - core}
        up, down = at(1, 0, 0), at(RING - 1, 0, 0)
        barrier = pltpu.get_barrier_semaphore()
        mates = [(dy, dx) for dy in (0, 1, 3) for dx in range(RING) if dy or dx]
        mates.sort(key=lambda m: (far(m[0]), -far(m[1])))
        near = [at(0, 0, o) for o in OTHERS] + [at(0, o, 0) for o in OTHERS] + [sibling]
        near += [at(o, 0, 0) for o in OTHERS] + [at(o, 0, 0) | sibling for o in OTHERS]
        for device in near:
            pl.semaphore_signal(barrier, inc=1, device_id=device)

        q_rows = n_q * qlen
        r = lax.broadcasted_iota(jnp.int32, (doc_rows, dlen), 0)
        c = lax.broadcasted_iota(jnp.int32, (doc_rows, dlen), 1)
        spread = jnp.where(r // n_docs == c, 1.0, 0.0).astype(jnp.bfloat16)
        loads[2].wait()
        qm = qm_ref[...].astype(jnp.float32)
        q_keep = jnp.concatenate([as_column(qm[i:i + 1], qlen) for i in range(n_q)], axis=0)

        both = sent.at[pl.ds(0, w.shape[0] + n_q * qlen * qh.shape[2] // w.shape[1])]
        pltpu.make_async_copy(both, both, load_sem.at[0]).wait()
        w_val = w[...]
        q_unit = unit_rows(qh[...].reshape(q_rows, qh.shape[2]), w_val)
        q_rows_ref[...] = jnp.where(q_keep > 0, q_unit, 0.0)
        for k in range(chunks):
            block = [q_rows_ref[pl.ds(k * (SLOT // n_q) + t, n_q, stride=qlen)] for t in range(SLOT // n_q)]
            qbuf[k, y, x] = jnp.concatenate(block, axis=0).astype(jnp.bfloat16)

        def query_copy(mate, rnd):
            ref = qbuf.at[pl.ds(rnd * (chunks // rounds), chunks // rounds), y, x]
            dy, t = mate[0], rnd * tiles // rounds
            sem = ROW0 if dy == 0 else NEAR0[t] if t == dy // 2 else NEAR1
            return pltpu.make_async_remote_copy(
                src_ref=ref, dst_ref=ref, send_sem=send, recv_sem=recv.at[sem], device_id=at(0, *mate))

        def arrived(sem, ref):
            pltpu.make_async_copy(ref, ref, recv.at[sem]).wait()

        def row_part(dy, t):
            return qbuf.at[pl.ds(t * RING, RING), (y + RING - dy) % RING]

        def row_copy(dy):
            ref = row_part(dy, 0 if dy == 1 else 1)
            return pltpu.make_async_remote_copy(
                src_ref=ref, dst_ref=ref, send_sem=send, recv_sem=recv.at[ROW2],
                device_id=at(0, dy, 0))

        loads[3].wait()
        pltpu.make_async_copy(dh_hbm, dh, load_sem.at[4]).wait()
        dm = dm_ref[...].astype(jnp.float32)
        lane = lax.broadcasted_iota(jnp.int32, dm.shape, 1)
        first = jnp.min(jnp.where(dm > 0, lane, dlen), axis=1, keepdims=True)
        r = lax.broadcasted_iota(jnp.int32, (n_docs, doc_rows), 1)
        d = lax.broadcasted_iota(jnp.int32, (n_docs, doc_rows), 0)
        pick = jnp.where(r == first * n_docs + d, 1.0, 0.0).astype(jnp.bfloat16)
        keep = lax.dot_general(spread, dm.astype(jnp.bfloat16), (((1,), (1,)), ((), ())),
                               preferred_element_type=jnp.float32)
        r = lax.broadcasted_iota(jnp.int32, keep.shape, 0)
        c = lax.broadcasted_iota(jnp.int32, keep.shape, 1)
        keep = jnp.sum(jnp.where(r % n_docs == c, keep, 0.0), axis=1, keepdims=True)
        cut = dlen // 5
        unit = jnp.concatenate([
            unit_rows(dh[i:i + cut].reshape(cut * n_docs, dh.shape[2]), w[...])
            for i in range(0, dlen, cut)], axis=0)
        unit = jnp.where(keep > 0, unit, 0.0).astype(jnp.bfloat16)
        valid = jnp.dot(pick, unit, preferred_element_type=jnp.float32)
        valid = jnp.concatenate([valid, valid], axis=0)
        valid = jnp.broadcast_to(valid[None], (doc_rows // 8, 8, valid.shape[1]))
        filled = jnp.where(keep > 0, unit.astype(jnp.float32), valid.reshape(doc_rows, valid.shape[2]))
        pbuf[z, core] = filled.astype(jnp.bfloat16)

        def doc_part(rel, h):
            return pbuf.at[(z + rel) % RING, core, parts[h]]

        def swap_copy(rel, h):
            ref = doc_part(rel, h)
            sem = SWAP0 if rel == 0 else SWAP2 if rel == 2 else SWAP1[rel // 2 == h]
            return pltpu.make_async_remote_copy(
                src_ref=ref, dst_ref=ref, send_sem=send, recv_sem=recv.at[sem], device_id=sibling)

        def z_copy(way, h):
            ref = doc_part(0, h)
            sem = SIDE1 if h < 2 else SIDE0[h - 3]
            return pltpu.make_async_remote_copy(
                src_ref=ref, dst_ref=ref, send_sem=send, recv_sem=recv.at[sem],
                device_id=down if way else up)

        def pass_copy(way, i):
            ref = doc_part(1 if way else RING - 1, 3 + 2 * way + i)
            return pltpu.make_async_remote_copy(
                src_ref=ref, dst_ref=ref, send_sem=send, recv_sem=recv.at[PASSED],
                device_id=down if way else up)

        loads[5].wait()
        pl.semaphore_wait(barrier, len(near))
        for off in OTHERS:
            pl.semaphore_signal(ready, inc=1, device_id=at(0, 0, off))
        for i in range(3):
            for way in range(2):
                z_copy(way, 1 - way if i == 2 else 3 + 2 * way + i).start()
        for rnd in range(rounds):
            for mate in mates:
                if 0 in mate:
                    query_copy(mate, rnd).start()
        swap_copy(0, 2).start()
        pl.semaphore_wait(ready, 3)
        for i in range(tiles):
            for rnd in range(rounds // tiles):
                for mate in mates:
                    if 0 not in mate:
                        t = i if mate[0] == 1 else 1 - i
                        query_copy(mate, t * (rounds // tiles) + rnd).start()

        sub = lax.broadcasted_iota(jnp.int32, (8, plane), 0)
        found, total = {}, {}

        def score(rel, swapped, part, spots):
            docs = pbuf[(z + rel) % RING, 1 - core if swapped else core, parts[part]]
            for dy, t in spots:
                q_tile = row_part(dy, t)[...].reshape(plane, qbuf.shape[-1])
                sim = lax.dot_general(docs, q_tile, (((1,), (1,)), ((), ())),
                                      preferred_element_type=jnp.float32)
                best = jnp.max(sim.reshape(docs.shape[0] // 8, 8, plane), axis=0)
                tile, key = (rel, swapped, dy, t), (rel, swapped, dy)
                if part < 2 and tile not in found:
                    found[tile] = best
                    continue
                if part < 2:
                    best = jnp.maximum(best, found[tile])
                best = jnp.maximum(best, pltpu.roll(best, 4, 0))
                total[key] = total[key] + best if key in total else best

        sides, row0 = ((0, 3), (1, 1)), ((0, 0), (0, 1))
        near0, near1, row2 = ((1, 0), (3, 1)), ((1, 1), (3, 0)), ((2, 0), (2, 1))
        docs_ref, row_ref = pbuf.at[z, core], qbuf.at[:, y]
        arrived(ROW0, row_ref.at[:, pl.ds(0, RING - 1)])
        arrived(SWAP0, docs_ref)
        score(0, 0, 2, row0)
        score(0, 1, 2, row0)
        for i in range(2):
            for way in range(2):
                z_copy(way, 3 + 2 * way + i).wait_recv()
                pass_copy(way, i).start()
                if i:
                    swap_copy(1 if way else 3, way).start()
        for way, rel in sides:
            score(rel, 0, way, row0)
        arrived(SIDE1, docs_ref)
        for way in range(2):
            swap_copy(1 if way else 3, 1 - way).start()
        arrived(SWAP1[0], docs_ref)
        arrived(NEAR0[0], row_part(1, 0))
        row_copy(1).start()
        arrived(NEAR0[1], row_part(3, 1))
        row_copy(3).start()
        for way, rel in sides:
            score(rel, 0, 1 - way, row0)
            score(rel, 1, way, row0)
        for spots in (near0, near1):
            if spots is near1:
                arrived(NEAR1, row_ref)
            score(0, 0, 2, spots)
            score(0, 1, 2, spots)
            for way, rel in sides:
                score(rel, 0, way, spots)
                score(rel, 1, way, spots)
                score(rel, 0, 1 - way, spots)
        arrived(PASSED, docs_ref)
        for way in range(2):
            swap_copy(2, way).start()
        arrived(SWAP1[1], docs_ref)
        for way, rel in sides:
            score(rel, 1, 1 - way, row0 + near0 + near1)
        score(2, 0, 2, row0 + near0 + near1)
        arrived(ROW2, row_ref)
        arrived(SWAP2, docs_ref)
        score(0, 0, 2, row2)
        score(0, 1, 2, row2)
        for way, rel in sides:
            for side in range(2):
                score(rel, side, way, row2)
                score(rel, side, 1 - way, row2)
        score(2, 0, 2, row2)
        score(2, 1, 2, row0 + near0 + near1 + row2)

        half = lax.broadcasted_iota(jnp.int32, (8, 128), 1) < 64
        for rel in range(RING):
            for dy in range(RING):
                s = jnp.where(sub < 4, total[rel, 0, dy], total[rel, 1, dy])
                s = s[:, :128] + s[:, 128:]
                sums[rel, (y + RING - dy) % RING] = s + pltpu.roll(s, 64, 1)
        temp = temp_ref[...]
        logits = []
        for rel in range(RING):
            s = jnp.concatenate([jnp.where(half, sums[rel, i], sums[rel, i + 1]) for i in (0, 2)], axis=1)
            s = s + pltpu.roll(s, n_q, 1)
            s = s + pltpu.roll(s, 2 * n_q, 1)
            logits.append(s / temp)
        peak = jnp.maximum(jnp.maximum(logits[0], logits[1]), jnp.maximum(logits[2], logits[3]))
        peak = jnp.max(peak, axis=0, keepdims=True)
        mass = sum(jnp.exp(g - peak) for g in logits)
        part = peak + jnp.log(jnp.sum(mass, axis=0, keepdims=True))
        lanes = lax.broadcasted_iota(jnp.int32, (8, plane), 1)
        is_own = (sub == lanes % n_q) & (lanes // SLOT == y * RING + x) & (lanes % SLOT >= SLOT - n_q)
        own = jnp.sum(jnp.where(is_own, logits[0], 0.0), axis=0, keepdims=True)
        own_sum = jnp.sum(own, axis=1, keepdims=True)
        slot = lax.broadcasted_iota(jnp.int32, (1, 128), 1) % SLOT

        def fold(row):
            return jnp.where(slot >= 12, row[:, :128], pltpu.roll(row[:, 128:], 128 - n_q, 1))

        row = jnp.where(slot >= 8, fold(part), own_sum)
        own = fold(own)
        here = core * RING ** 3 + me
        pieces[here] = row

        def tell(across, dz, dy, dx):
            other = at(dz, dy, dx) | {'data2': 1 - core if across else core}
            return pltpu.make_async_remote_copy(
                src_ref=pieces.at[here], dst_ref=pieces.at[here], send_sem=rsend, recv_sem=rrecv,
                device_id=other)

        rest = [(a, i, j, k) for a in range(2) for i in range(RING) for j in range(RING) for k in range(RING)]
        for a, i, j, k in sorted(rest[1:], key=lambda o: (-far(*o[1:]), -o[0])):
            tell(a, i, j, k).start()
        everyone = pieces.at[pl.ds(0, n_dev - 1)]
        pltpu.make_async_copy(everyone, everyone, rrecv).wait()
        ls = pieces[...].reshape(2 * RING, RING * RING, 128)
        peak = jnp.max(ls, axis=1, keepdims=True)
        mass = jnp.sum(jnp.exp(ls - peak), axis=1)
        whole = peak.reshape(2 * RING, 128) + jnp.log(mass)
        slot = lax.broadcasted_iota(jnp.int32, whole.shape, 1) % SLOT
        answer = jnp.where(slot >= 8, whole, 0.0)
        lane = lax.broadcasted_iota(jnp.int32, whole.shape, 1)
        answer = answer - jnp.where(lane == 0, jnp.sum(ls, axis=1), 0.0)
        answer = jnp.sum(jnp.sum(answer, axis=1, keepdims=True), axis=0, keepdims=True)
        group = lax.broadcasted_iota(jnp.int32, whole.shape, 0)
        losses = jnp.sum(jnp.where(group == core * RING + z, whole, 0.0), axis=0, keepdims=True)
        losses = losses - own
        spot = (y * RING + x) % 8 * SLOT + jnp.where(y >= 2, 8, 12)
        losses = pltpu.roll(jnp.broadcast_to(losses, (8, 128)), (128 - spot) % 128, 1)
        out_ref[0:1] = losses[0:1]
        out_ref[1:2] = jnp.broadcast_to(answer / (n_dev * n_q), (1, 128))

        pltpu.make_async_copy(sent, sent, send).wait()
        pltpu.make_async_copy(everyone, everyone, rsend).wait()

    return kernel


def hand_over(found_ref, loss_ref, mean_ref):
    loss_ref[...] = found_ref[0:1, :loss_ref.shape[1]]
    mean_ref[...] = found_ref[1:2, 0:1]


def solution(mesh):
    row_spec = P(('replica', 'data2', 'data'))
    tok_spec = P(('replica', 'data2', 'data'), None, None)
    mask_spec = P(('replica', 'data2', 'data'), None)

    def local_step(query_hidden, doc_hidden, w_proj, query_mask, doc_mask, temperature):
        n_q, qlen, hidden = query_hidden.shape
        n_docs, dlen, _ = doc_hidden.shape
        proj = w_proj.shape[1]
        chunks = n_q * qlen // SLOT
        sent_rows = (RING * (RING - 1) - 1 + RING) * n_q * qlen + 7 * n_docs * dlen
        dma = pltpu.SemaphoreType.DMA
        found = pl.pallas_call(
            make_kernel(n_docs, dlen, n_q, qlen),
            out_shape=pltpu.VMEM((2, 128), jnp.float32),
            in_specs=[pl.BlockSpec(memory_space=pl.ANY)] * 6,
            out_specs=pl.BlockSpec(memory_space=pltpu.VMEM),
            scratch_shapes=[
                pltpu.VMEM(query_hidden.shape, jnp.bfloat16),
                pltpu.VMEM((dlen, n_docs, hidden), jnp.bfloat16),
                pltpu.VMEM(w_proj.shape, jnp.bfloat16),
                pltpu.VMEM(query_mask.shape, jnp.int32),
                pltpu.VMEM(doc_mask.shape, jnp.int32),
                pltpu.VMEM((1, 1), jnp.float32),
                pltpu.VMEM((chunks, RING, RING, SLOT, proj), jnp.bfloat16),
                pltpu.VMEM((RING, 2, n_docs * dlen, proj), jnp.bfloat16),
                pltpu.VMEM((RING, RING, 8, 128), jnp.float32),
                pltpu.VMEM((2 * RING ** 3, 1, 128), jnp.float32),
                pltpu.VMEM((sent_rows, proj), jnp.bfloat16),
                pltpu.VMEM((n_q * qlen, proj), jnp.float32),
                dma((5,)), dma, dma((15,)), dma, dma,
                pltpu.SemaphoreType.REGULAR,
            ],
            compiler_params=pltpu.CompilerParams(collective_id=0, has_side_effects=True),
        )(query_hidden, jnp.transpose(doc_hidden, (1, 0, 2)), w_proj, query_mask, doc_mask,
          temperature.reshape(1, 1))
        losses, mean = pl.pallas_call(
            hand_over,
            out_shape=(jax.ShapeDtypeStruct((1, n_q), jnp.float32),
                       jax.ShapeDtypeStruct((1, 1), jnp.float32)),
            in_specs=[pl.BlockSpec(memory_space=pltpu.VMEM)],
            out_specs=(pl.BlockSpec(memory_space=pltpu.VMEM),) * 2,
            compiler_params=pltpu.CompilerParams(vmem_limit_bytes=2 ** 20))(found)
        return losses.reshape(n_q), mean.reshape(1)

    return jax.shard_map(local_step, mesh=mesh,
                         in_specs=(tok_spec, tok_spec, P(None, None), mask_spec, mask_spec, P()),
                         out_specs=(row_spec, P('replica')), check_vma=False)
```
